256 devices in a mesh: sec: 2 (over core), grp: 4 (over x), cp: 32 (over z, y).
Axes of the slice: x: 4, y: 4, z: 8, core: 2. Of those that a mesh axis runs over, the one named last changes fastest.
Arguments:
- prompt_states: bfloat16 [8, 6144, 8192], P('grp', 'cp'), may hold values from -6 to 6
- prompt_queries: bfloat16 [8, 6144, 1024], P('grp', 'cp', 'sec'), may hold values from -180 to 180
- decode_states: bfloat16 [3, 128, 8192], P(None, 'grp'), may hold values from -6 to 6
- decode_queries: bfloat16 [3, 128, 1024], P(None, 'grp', 'sec'), may hold values from -180 to 180
- latent_down: bfloat16 [8192, 256], P(None, 'sec'), may hold values from -0.0625 to 0.0625
- key_up: bfloat16 [128, 1024], P(None, 'sec'), may hold values from -0.5 to 0.5
- value_up: bfloat16 [128, 1024], P(None, 'sec'), may hold values from -0.5 to 0.5
- prompt_lengths: int32 [8], P('grp'), may hold values from 1536 to 6144
- block_order: int32 [64], replicated, may hold values from 0 to 63, each once
- page_owner: int32 [4, 32, 24], P('grp'), may hold values from 0 to 31, as said below
- decode_context: int32 [128], P('grp'), may hold values from 768 to 6144
Outputs:
- prefill_out: bfloat16 [8, 6144, 1024], P('grp', 'cp', 'sec')
- decode_out: bfloat16 [3, 128, 1024], P(None, 'grp', 'sec')
- page_cache: bfloat16 [4, 32, 384, 256], P('grp', 'cp')
The draws below stay inside these ranges and needn't reach their ends.
Inputs may be any that keep to these rules, and one draw needn't show every extreme that they name: block_order names each block of a prompt once. page_owner[g, s, k] is an index along cp; every owner receives exactly 24 pages of its group, and at most 1 from one device.
All inputs are finite; a program needn't handle non-finite values.
Results may differ from the reference program's by a relative error of at most 0.012.
The reference program's roundings to bfloat16 on the way count: a program that leaves them out, or rounds other values in their place, can miss the bound.
Values may be sent and summed in bfloat16 or wider, within the bound.
No kernel may reach another device: no remote copies, remote signals or barrier semaphores. Data moves between devices by JAX's collectives and lax.ppermute only.
A program may use at most 128 MiB of HBM per device.

```python
import jax
import jax.numpy as jnp
from jax import lax

D = 8192
HEADS = 8
HEAD = 128
RANK = 128
BLOCK = 96
PAGE = 16
PPG = 2
ROW_GRP = 32
STEPS = 3
SEQ = 6144
PROMPTS = 8
ROWS = 128
PAGES_DEV = 24
GROUPS = 4
OWNERS = 32
BLOCKS = 64


def spread_queries(draw_key, out_shape):
    base_key = jax.random.fold_in(draw_key, 0)
    return jnp.clip(2.5 * jax.random.normal(base_key, out_shape, jnp.float32), -20.0, 20.0).astype(jnp.bfloat16)


def draw_prompt_queries(key, part):
    return spread_queries(jax.random.fold_in(key, 11), (PROMPTS, SEQ, HEADS * HEAD))


def draw_decode_queries(key, part):
    return spread_queries(jax.random.fold_in(key, 23), (STEPS, ROWS, HEADS * HEAD))


def draw_page_owner(key, part):
    group_key, page_key = jax.random.split(jax.random.fold_in(key, 37))
    owner_perm = jax.vmap(lambda one_key: jax.random.permutation(one_key, OWNERS))(jax.random.split(group_key, GROUPS))
    page_perm = jax.vmap(lambda one_key: jax.random.permutation(one_key, PAGES_DEV))(jax.random.split(page_key, GROUPS * OWNERS))
    page_perm = page_perm.reshape(GROUPS, OWNERS, PAGES_DEV).astype(jnp.int32)
    shifted = (jnp.arange(OWNERS, dtype=jnp.int32)[None, :, None] + page_perm) % OWNERS
    spread = jnp.broadcast_to(owner_perm.astype(jnp.int32)[:, None, :], (GROUPS, OWNERS, OWNERS))
    return jnp.take_along_axis(spread, shifted, axis=2).astype(jnp.int32)


def with_ends(result, key, least, largest):
    longest = result.shape.index(max(result.shape))
    spots = []
    for shift in (0, 1):
        where = [jax.random.randint(jax.random.fold_in(key, axis), (), 0, length) for axis, length in enumerate(result.shape)]
        where[longest] = (where[longest] + shift) % result.shape[longest]
        spots.append(tuple(where))
    return result.at[spots[0]].set(least).at[spots[1]].set(largest)


def steps_of(rng, shape, shards, least, top_value):
    def one(axis_at, shards_of):
        draws = jax.random.uniform(jax.random.fold_in(jax.random.fold_in(rng, 6), axis_at), (shards_of,), jnp.float32, least / len(shards), top_value / len(shards))
        return jnp.repeat(jnp.exp(draws), shape[axis_at] // shards_of).reshape((-1,) + (1,) * (len(shape) - axis_at - 1))

    gain = one(*shards[0])
    for cut in shards[1:]:
        gain = gain * one(*cut)
    return gain


def normal_values(rng, dims, scale, limit, pieces=(), kind=jnp.bfloat16):
    array = scale * jax.random.normal(rng, dims, jnp.float32)
    if pieces:
        array = array * steps_of(rng, dims, pieces, -0.22, 0.18)
    return jnp.clip(array, -limit, limit).astype(kind)


def setup_inputs(seed: int = 0) -> dict:
    splits = jax.random.split(jax.random.key(seed), 12)
    prompt_states = normal_values(splits[0], (PROMPTS, SEQ, D), 1.0, 6.0, ((0, 4), (1, 32)))
    prompt_queries = draw_prompt_queries(jax.random.fold_in(splits[11], 71), 0)
    decode_states = normal_values(splits[2], (STEPS, ROWS, D), 1.0, 6.0, ((1, 4),))
    decode_queries = draw_decode_queries(jax.random.fold_in(splits[11], 71), 0)
    latent_down = normal_values(splits[4], (D, 2 * RANK), D ** -0.5, 0.0625, ((1, 2),))
    key_up = normal_values(splits[5], (RANK, HEADS * HEAD), RANK ** -0.5, 0.5, ((1, 2),))
    value_up = normal_values(splits[6], (RANK, HEADS * HEAD), RANK ** -0.5, 0.5, ((1, 2),))
    prompt_lengths = with_ends(jax.random.randint(splits[7], (PROMPTS,), SEQ // 4, SEQ + 1), jax.random.fold_in(splits[7], 1), SEQ // 4, SEQ).astype(jnp.int32)
    block_order = jax.random.permutation(splits[8], BLOCKS).astype(jnp.int32)
    page_owner = draw_page_owner(jax.random.fold_in(splits[11], 71), 0)
    decode_context = with_ends(jax.random.randint(splits[10], (ROWS,), SEQ // 8, SEQ + 1), jax.random.fold_in(splits[10], 1), SEQ // 8, SEQ).astype(jnp.int32)
    return {"prompt_states": prompt_states, "prompt_queries": prompt_queries, "decode_states": decode_states, "decode_queries": decode_queries, "latent_down": latent_down, "key_up": key_up, "value_up": value_up, "prompt_lengths": prompt_lengths, "block_order": block_order, "page_owner": page_owner, "decode_context": decode_context}


NEG = -1e30


def stored_positions(block_order, stored_rows):
    return block_order[stored_rows // BLOCK] * BLOCK + stored_rows % BLOCK


def absorb(queries, key_up):
    row_count = queries.shape[0]
    q_parts = queries.astype(jnp.float32).reshape(row_count, HEADS, HEAD)
    u_parts = key_up.astype(jnp.float32).reshape(RANK, HEADS, HEAD)
    return jnp.einsum("nhd,rhd->hnr", q_parts, u_parts).astype(jnp.bfloat16)


def rebuild(latent_out, value_up):
    u_parts = value_up.astype(jnp.float32).reshape(RANK, HEADS, HEAD)
    rebuilt = jnp.einsum("hnr,rhd->nhd", latent_out.astype(jnp.float32), u_parts)
    return rebuilt.astype(jnp.bfloat16).reshape(latent_out.shape[1], HEADS * HEAD)


def attend(query_abs, key_rows, value_rows, key_mask):
    scores = jnp.dot(query_abs, key_rows.T, preferred_element_type=jnp.float32) * HEAD ** -0.5
    scores = jnp.where(key_mask, scores, NEG)
    row_peak = jnp.max(scores, axis=-1, keepdims=True)
    weights = jnp.where(key_mask, jnp.exp(scores - row_peak), 0.0)
    row_total = jnp.sum(weights, axis=-1, keepdims=True)
    weighted = jnp.dot(weights.astype(jnp.bfloat16), value_rows, preferred_element_type=jnp.float32)
    return (weighted / row_total).astype(jnp.bfloat16)


def reference(prompt_states, prompt_queries, decode_states, decode_queries, latent_down, key_up, value_up, prompt_lengths, block_order, page_owner, decode_context):
    latent = jnp.dot(prompt_states.reshape(PROMPTS * SEQ, D), latent_down, preferred_element_type=jnp.float32).astype(jnp.bfloat16).reshape(PROMPTS, SEQ, 2 * RANK)
    new_latent = jnp.dot(decode_states.reshape(STEPS * ROWS, D), latent_down, preferred_element_type=jnp.float32).astype(jnp.bfloat16).reshape(STEPS, ROWS, 2 * RANK)
    positions = stored_positions(block_order, jnp.arange(SEQ, dtype=jnp.int32))
    causal = positions[None, :] <= positions[:, None]

    def prefill_prompt(prompt_id):
        prompt_latent = latent[prompt_id]
        query_abs = absorb(prompt_queries[prompt_id], key_up)

        def one_head(head_abs):
            return attend(head_abs, prompt_latent[:, :RANK], prompt_latent[:, RANK:], causal)

        latent_out = lax.map(one_head, query_abs)
        rebuilt = rebuild(latent_out, value_up)
        live_rows = positions < prompt_lengths[prompt_id]
        return jnp.where(live_rows[:, None], rebuilt, jnp.zeros_like(rebuilt))

    prefill_out = lax.map(prefill_prompt, jnp.arange(PROMPTS, dtype=jnp.int32))

    step_ids = jnp.arange(STEPS, dtype=jnp.int32)
    own_mask = step_ids[None, :] <= step_ids[:, None]

    def decode_row(row_id):
        group_id = row_id // ROW_GRP
        prompt_id = group_id * PPG + (row_id % ROW_GRP) // (ROW_GRP // PPG)
        row_limit = jnp.minimum(decode_context[row_id], prompt_lengths[prompt_id])
        key_rows = jnp.concatenate([latent[prompt_id], new_latent[:, row_id]], axis=0)
        cache_mask = jnp.broadcast_to((positions < row_limit)[None, :], (STEPS, SEQ))
        key_mask = jnp.concatenate([cache_mask, own_mask], axis=1)
        query_abs = absorb(decode_queries[:, row_id], key_up)
        latent_out = jax.vmap(lambda head_abs: attend(head_abs, key_rows[:, :RANK], key_rows[:, RANK:], key_mask))(query_abs)
        return rebuild(latent_out, value_up)

    decode_out = jnp.transpose(lax.map(decode_row, jnp.arange(ROWS, dtype=jnp.int32)), (1, 0, 2))

    flat_owner = page_owner.reshape(GROUPS, OWNERS * PAGES_DEV)
    ranked = jnp.argsort(flat_owner, axis=1, stable=True).astype(jnp.int32)
    source = ranked // PAGES_DEV
    local_page = ranked % PAGES_DEV
    per_prompt = 2 * BLOCK // PAGE
    prompt_index = jnp.arange(GROUPS, dtype=jnp.int32)[:, None] * PPG + local_page // per_prompt
    first_row = source * (2 * BLOCK) + (local_page % per_prompt) * PAGE
    rows_index = first_row[..., None] + jnp.arange(PAGE, dtype=jnp.int32)
    page_cache = latent[prompt_index[..., None], rows_index].reshape(GROUPS, OWNERS, PAGES_DEV * PAGE, 2 * RANK)
    return prefill_out, decode_out, page_cache
```

```python
import functools
import math

import jax
import jax.numpy as jnp
import numpy as np
from jax import lax
from jax.experimental import pallas as pl
from jax.experimental.pallas import tpu as pltpu
from jax.sharding import PartitionSpec as P


HEAD = 128
RANK = 128
HEADS = 4
BLOCK = 96
PAGE = 16
PPG = 2
ROW_GRP = 32
HALF_GRP = ROW_GRP // PPG
STEPS = 3
PAGES_DEV = 24
ZN, YN = 8, 4
CP = ZN * YN
UNITS = 4
QL = HEADS * BLOCK
DH = 64
DL = HEADS * DH
G = 4
GK = G * BLOCK
NEG = -1e30
SCALE2 = math.log2(math.e) / math.sqrt(HEAD)

CHUNK_Z = [[0], [7, 1], [6, 2], [5, 3], [4]]
SLOT_Z = np.zeros((5, 16), np.int32)
SLOT_Y = np.zeros((5, 16), np.int32)
SLOT_A = np.zeros((5, 16), np.int32)
SLOT_ROW = np.zeros((5, 16), np.int32)
SLOT_OK = np.zeros((5, 16), bool)
for _c, _zs in enumerate(CHUNK_Z):
    for _i, _dz in enumerate(_zs):
        for _dy in range(YN):
            for _a in range(2):
                _j = _i * 8 + _dy * 2 + _a
                SLOT_Z[_c, _j], SLOT_Y[_c, _j], SLOT_A[_c, _j] = _dz, _dy, _a
                SLOT_ROW[_c, _j] = _i * 16 + _dy * 4 + _a
                SLOT_OK[_c, _j] = True

M_IDX, M_ORD, M_STRICT, M_ALL, M_DEC, M_OWN, M_LEN, M_POS = 0, 16, 32, 34, 36, 37, 39, 41
PG_HAS, PG_K, PG_SLOT = 0, 1, 2


def lookup(table, indices):
    matches = indices[..., None] == jnp.arange(table.shape[0], dtype=jnp.int32)
    return jnp.sum(jnp.where(matches, table, 0), axis=-1)


def scalar_tables(block_order, lengths, contexts, owners, ci, sec):
    z, y = ci // YN, ci % YN
    source = ((z + SLOT_Z) % ZN) * YN + (y + SLOT_Y) % YN
    order = lookup(block_order, 2 * source + SLOT_A)
    order = jnp.where(SLOT_OK, order, 4096 + np.arange(16, dtype=np.int32))
    rank = jnp.sum((order[:, None, :] < order[:, :, None]).astype(jnp.int32), axis=-1)
    place = rank[:, None, :] == np.arange(16, dtype=np.int32)[None, :, None]
    idx = jnp.sum(jnp.where(place, SLOT_ROW[:, None, :], 0), axis=-1)
    ranked = jnp.sum(jnp.where(place, order[:, None, :], 0), axis=-1)
    own = lookup(block_order, 2 * ci + np.arange(2, dtype=np.int32))
    alive = own * BLOCK < jnp.max(lengths)
    strict = jnp.sum((order[:, None, :] < own[None, :, None]) & alive[None, :, None], axis=-1)
    every = jnp.sum((order[:, None, :] <= own[None, :, None]) & alive[None, :, None], axis=-1)
    row_prompt = np.arange(ROW_GRP, dtype=np.int32) // HALF_GRP
    limits = jnp.minimum(contexts, jnp.where(row_prompt == 0, lengths[0], lengths[1]))
    dec = jnp.sum(order * BLOCK < jnp.max(limits), axis=-1, keepdims=True)
    spread = jnp.broadcast_to(
        jnp.concatenate([own, lengths, jnp.stack([z, y, sec])])[None], (5, 7)
    )
    meta = jnp.concatenate(
        [idx, ranked, strict.astype(jnp.int32), every.astype(jnp.int32), dec.astype(jnp.int32), spread],
        axis=1,
    ).astype(jnp.int32)
    mine = owners == ci
    has = jnp.sum(mine.astype(jnp.int32), axis=1)
    page = jnp.sum(jnp.where(mine, np.arange(PAGES_DEV, dtype=np.int32), 0), axis=1)
    before = np.arange(CP)[None, :] < np.arange(CP)[:, None]
    slot = jnp.sum(jnp.where(before, has[None, :], 0), axis=1)
    pages = jnp.stack([has, page, slot]).astype(jnp.int32)
    limit_rows = limits.reshape(PPG, 1, 1, HALF_GRP)
    limit_lanes = jnp.broadcast_to(limit_rows, (PPG, HEADS, STEPS, HALF_GRP)).reshape(PPG, HEADS, 48)
    limit_lanes = jnp.pad(limit_lanes, ((0, 0), (0, 0), (0, DH - 48))).reshape(PPG, 1, DL)
    return meta, pages, limit_lanes


def queries_kernel(q_ref, dq_ref, u_ref, qt_ref, dqt_ref):
    for p in range(PPG):
        for a in range(2):
            rows = []
            for h in range(HEADS):
                cols = slice(h * HEAD, (h + 1) * HEAD)
                rows.append(
                    lax.dot_general(
                        q_ref[p, a * BLOCK : (a + 1) * BLOCK, cols],
                        u_ref[:, cols],
                        (((1,), (1,)), ((), ())),
                        preferred_element_type=jnp.float32,
                    )
                )
            qt_ref[p * 2 + a] = jnp.concatenate(rows, axis=0).T.astype(jnp.bfloat16)
        rows = []
        for h in range(HEADS):
            cols = slice(h * HEAD, (h + 1) * HEAD)
            q = jnp.concatenate(
                [dq_ref[t, p * HALF_GRP : (p + 1) * HALF_GRP, cols] for t in range(STEPS)]
                + [jnp.zeros((HALF_GRP, HEAD), jnp.bfloat16)],
                axis=0,
            )
            rows.append(
                lax.dot_general(
                    q, u_ref[:, cols], (((1,), (1,)), ((), ())), preferred_element_type=jnp.float32
                )
            )
        dqt_ref[p] = jnp.concatenate(rows, axis=0).T.astype(jnp.bfloat16)


def prepare_queries(prompt_queries, decode_queries, key_up):
    return pl.pallas_call(
        queries_kernel,
        out_shape=(
            jax.ShapeDtypeStruct((UNITS, RANK, QL), jnp.bfloat16),
            jax.ShapeDtypeStruct((PPG, RANK, DL), jnp.bfloat16),
        ),
        cost_estimate=pl.CostEstimate(flops=10**9, bytes_accessed=10**6, transcendentals=0),
        name="queries",
    )(prompt_queries, decode_queries, key_up)


def softmax_step(k, v, q, keep, m_ref, l_ref, acc_ref, at):
    s = jnp.dot(k, q, preferred_element_type=jnp.float32) * SCALE2
    if keep is not None:
        s = jnp.where(keep, s, NEG)
    old = m_ref[at]
    new = jnp.maximum(old, jnp.max(s, axis=0, keepdims=True))
    factor = jnp.exp2(old - new)
    w = jnp.exp2(s - new)
    m_ref[at] = new
    l_ref[at] = l_ref[at] * factor + jnp.sum(w, axis=0, keepdims=True)
    part = lax.dot_general(
        v, w.astype(jnp.bfloat16), (((0,), (0,)), ((), ())), preferred_element_type=jnp.float32
    )
    acc_ref[at] = acc_ref[at] * factor + part


def chunk_kernel(chunk, n_src, sizes, first, last, *refs):
    refs = list(refs)
    meta = refs.pop(0)
    pages = refs.pop(0) if last else None
    mine = [refs.pop(0) for _ in range(n_src)]
    theirs = [refs.pop(0) for _ in range(n_src)]
    qt, dqt, limit = refs.pop(0), refs.pop(0), refs.pop(0)
    if first:
        new_mine, new_theirs = refs.pop(0), refs.pop(0)
    else:
        state_in = [refs.pop(0) for _ in range(6)]
    if last:
        others = [(refs.pop(0), refs.pop(0)) for _ in range(7)]
        vup = refs.pop(0)
        out_ref, dec_ref, cache_ref = refs.pop(0), refs.pop(0), refs.pop(0)
    else:
        state_out = [refs.pop(0) for _ in range(6)]
    kbuf, vbuf, sems = refs.pop(0), refs.pop(0), refs.pop(0)
    if last:
        page_sems = refs.pop(0)
        state = state_in
    else:
        state = state_out
    m, l, acc, dm, dl, dacc = state

    sec = meta[chunk, M_POS + 2]
    spans, at = [], 0
    for n in sizes:
        spans.append((at, n))
        at += n

    def copies(k_src, v_src):
        made = []
        for i, (start, n) in enumerate(spans):
            made.append(pltpu.make_async_copy(k_src[i], kbuf.at[pl.ds(start, n)], sems.at[2 * i]))
            made.append(pltpu.make_async_copy(v_src[i], vbuf.at[pl.ds(start, n)], sems.at[2 * i + 1]))
        return made

    @pl.when(sec == 0)
    def _():
        for copy in copies(mine, theirs):
            copy.start()

    @pl.when(sec != 0)
    def _():
        for copy in copies(theirs, mine):
            copy.start()

    if last:
        z, y = meta[chunk, M_POS], meta[chunk, M_POS + 1]
        table = [(0, dy, others[0][0].at[dy], others[0][1].at[dy]) for dy in range(YN)]
        for i, dz in enumerate([7, 1, 6, 2, 5, 3]):
            table += [(dz, dy, others[1 + i][0].at[dy], others[1 + i][1].at[dy]) for dy in range(YN)]
        for i in range(2):
            table += [(4, 2 * i + e, mine[i].at[pl.ds(e * 4, 4)], theirs[i].at[pl.ds(e * 4, 4)]) for e in range(2)]

        def page_copies(n, dz, dy, own_src, far_src):
            s = lax.rem(z + dz, ZN) * YN + lax.rem(y + dy, YN)
            page, slot = pages[PG_K, s], pages[PG_SLOT, s]
            block, row = page // 6, pl.multiple_of(lax.rem(page, 6) * PAGE, PAGE)
            rows = pl.ds(pl.multiple_of(jnp.minimum(slot, PAGES_DEV - 1) * PAGE, PAGE), PAGE)
            own_at, far_at = sec * RANK, (1 - sec) * RANK
            return (
                pages[PG_HAS, s] > 0,
                pltpu.make_async_copy(
                    own_src.at[block, pl.ds(row, PAGE), :],
                    cache_ref.at[rows, pl.ds(pl.multiple_of(own_at, RANK), RANK)],
                    page_sems.at[2 * n],
                ),
                pltpu.make_async_copy(
                    far_src.at[block, pl.ds(row, PAGE), :],
                    cache_ref.at[rows, pl.ds(pl.multiple_of(far_at, RANK), RANK)],
                    page_sems.at[2 * n + 1],
                ),
            )

        for n, entry in enumerate(table):
            has, one, two = page_copies(n, *entry)

            @pl.when(has)
            def _(one=one, two=two):
                one.start()
                two.start()

    if first:
        m[...] = jnp.full(m.shape, NEG, jnp.float32)
        l[...] = jnp.zeros(l.shape, jnp.float32)
        acc[...] = jnp.zeros(acc.shape, jnp.float32)
        is_key = sec == 0
        lane = lax.broadcasted_iota(jnp.int32, (1, DL), 1)
        step_of = lax.rem(lane, DH) // HALF_GRP
        for p in range(PPG):
            scores, values = [], []
            for t in range(STEPS):
                rows = slice(t * ROW_GRP + p * HALF_GRP, t * ROW_GRP + (p + 1) * HALF_GRP)
                a, b = new_mine[rows, :].astype(jnp.float32), new_theirs[rows, :].astype(jnp.float32)
                k, v = jnp.where(is_key, a, b), jnp.where(is_key, b, a)
                k = jnp.concatenate([k] * (DL // HALF_GRP), axis=0).T
                values.append(jnp.concatenate([v] * (DL // HALF_GRP), axis=0).T)
                s = jnp.sum(dqt[p].astype(jnp.float32) * k, axis=0, keepdims=True) * SCALE2
                scores.append(jnp.where(t <= step_of, s, NEG))
            peak = jnp.maximum(jnp.maximum(scores[0], scores[1]), scores[2])
            weights = [jnp.exp2(s - peak) for s in scores]
            dm[p] = peak
            dl[p] = weights[0] + weights[1] + weights[2]
            total = jnp.zeros((RANK, DL), jnp.float32)
            for w, v in zip(weights, values):
                total = total + w.astype(jnp.bfloat16).astype(jnp.float32) * v
            dacc[p] = total
    elif not last:
        for src, dst in zip(state_in, state_out):
            dst[...] = src[...]

    for copy in copies(mine, theirs):
        copy.wait()

    def rows_of(buf, g, p):
        return jnp.concatenate([buf[meta[chunk, M_IDX + g * G + j] + 2 * p] for j in range(G)], axis=0)

    key_row = lax.broadcasted_iota(jnp.int32, (BLOCK, QL), 0)
    query_row = lax.rem(lax.broadcasted_iota(jnp.int32, (BLOCK, QL), 1), BLOCK)
    behind = key_row - query_row
    for a in range(2):
        strict, every = meta[chunk, M_STRICT + a], meta[chunk, M_ALL + a]
        plain = strict // G

        def plain_step(g, carry, a=a):
            for p in range(PPG):
                at = p * 2 + a
                softmax_step(rows_of(kbuf, g, p), rows_of(vbuf, g, p), qt[at], None, m, l, acc, at)
            return carry

        lax.fori_loop(0, plain, plain_step, 0)

        @pl.when(every > plain * G)
        def _(a=a, plain=plain):
            own = meta[chunk, M_OWN + a]
            keep = jnp.concatenate(
                [behind + (meta[chunk, M_ORD + plain * G + j] - own) * BLOCK <= 0 for j in range(G)],
                axis=0,
            )
            for p in range(PPG):
                at = p * 2 + a
                softmax_step(rows_of(kbuf, plain, p), rows_of(vbuf, plain, p), qt[at], keep, m, l, acc, at)

    dec_row = lax.broadcasted_iota(jnp.int32, (BLOCK, DL), 0)

    def dec_step(g, carry):
        for p in range(PPG):
            keep = jnp.concatenate(
                [dec_row + meta[chunk, M_ORD + g * G + j] * BLOCK < limit[p] for j in range(G)], axis=0
            )
            softmax_step(rows_of(kbuf, g, p), rows_of(vbuf, g, p), dqt[p], keep, dm, dl, dacc, p)
        return carry

    lax.fori_loop(0, (meta[chunk, M_DEC] + G - 1) // G, dec_step, 0)

    if last:
        row = lax.broadcasted_iota(jnp.int32, (BLOCK, HEAD), 0)
        for p in range(PPG):
            for a in range(2):
                at = p * 2 + a
                o = (acc[at] / l[at]).T.astype(jnp.bfloat16)
                live = row + meta[chunk, M_OWN + a] * BLOCK < meta[chunk, M_LEN + p]
                for h in range(HEADS):
                    cols = slice(h * HEAD, (h + 1) * HEAD)
                    r = jnp.dot(
                        o[h * BLOCK : (h + 1) * BLOCK], vup[:, cols], preferred_element_type=jnp.float32
                    )
                    out_ref[p, a * BLOCK : (a + 1) * BLOCK, cols] = jnp.where(live, r, 0.0).astype(
                        jnp.bfloat16
                    )
            o = (dacc[p] / dl[p]).T.astype(jnp.bfloat16)
            for h in range(HEADS):
                cols = slice(h * HEAD, (h + 1) * HEAD)
                r = jnp.dot(
                    o[h * DH : (h + 1) * DH], vup[:, cols], preferred_element_type=jnp.float32
                ).astype(jnp.bfloat16)
                for t in range(STEPS):
                    dec_ref[t, p * HALF_GRP : (p + 1) * HALF_GRP, cols] = r[t * HALF_GRP : (t + 1) * HALF_GRP]
        for n, entry in enumerate(table):
            has, one, two = page_copies(n, *entry)

            @pl.when(has)
            def _(one=one, two=two):
                one.wait()
                two.wait()


STATE = (
    jax.ShapeDtypeStruct((UNITS, 1, QL), jnp.float32),
    jax.ShapeDtypeStruct((UNITS, 1, QL), jnp.float32),
    jax.ShapeDtypeStruct((UNITS, RANK, QL), jnp.float32),
    jax.ShapeDtypeStruct((PPG, 1, DL), jnp.float32),
    jax.ShapeDtypeStruct((PPG, 1, DL), jnp.float32),
    jax.ShapeDtypeStruct((PPG, RANK, DL), jnp.float32),
)


def attend_chunk(chunk, meta, mine, theirs, qt, dqt, limit, state=None, new=None, ending=None):
    first, last = state is None, ending is not None
    smem, vmem = pl.BlockSpec(memory_space=pltpu.SMEM), pl.BlockSpec(memory_space=pltpu.VMEM)
    anywhere = pl.BlockSpec(memory_space=pl.ANY)
    sizes = [a.size // (BLOCK * RANK) for a in mine]
    flat = [a.reshape(-1, BLOCK, RANK) for a in [*mine, *theirs]]
    args, specs = [meta], [smem]
    if last:
        args, specs = args + [ending["pages"]], specs + [smem]
    args, specs = args + flat, specs + [anywhere] * len(flat)
    args, specs = args + [qt, dqt, limit], specs + [vmem] * 3
    if first:
        args, specs = args + list(new), specs + [vmem] * 2
    else:
        args, specs = args + list(state), specs + [vmem] * 6
    rows = sum(sizes)
    scratch = [
        pltpu.VMEM((rows, BLOCK, RANK), jnp.bfloat16),
        pltpu.VMEM((rows, BLOCK, RANK), jnp.bfloat16),
        pltpu.SemaphoreType.DMA((2 * len(mine),)),
    ]
    if last:
        for pair in ending["others"]:
            args, specs = args + list(pair), specs + [anywhere] * 2
        args, specs = args + [ending["value_up"]], specs + [vmem]
        shapes = (
            jax.ShapeDtypeStruct((PPG, 2 * BLOCK, HEADS * HEAD), jnp.bfloat16),
            jax.ShapeDtypeStruct((STEPS, ROW_GRP, HEADS * HEAD), jnp.bfloat16),
            jax.ShapeDtypeStruct((PAGES_DEV * PAGE, 2 * RANK), jnp.bfloat16),
        )
        scratch.append(pltpu.SemaphoreType.DMA((2 * CP,)))
    else:
        shapes = STATE
    work = rows * BLOCK * (2 * QL + DL) * RANK * 4
    return pl.pallas_call(
        functools.partial(chunk_kernel, chunk, len(mine), sizes, first, last),
        out_shape=shapes,
        in_specs=specs,
        out_specs=[vmem] * len(shapes),
        scratch_shapes=scratch,
        cost_estimate=pl.CostEstimate(flops=2 * work, bytes_accessed=4 * 10**6, transcendentals=work // 512),
        compiler_params=pltpu.CompilerParams(vmem_limit_bytes=48 * 2**20),
        name=f"attend{chunk}",
    )(*args)


def shifted(x, dz, dy):
    pairs = [
        (z * YN + y, ((z + dz) % ZN) * YN + (y + dy) % YN) for z in range(ZN) for y in range(YN)
    ]
    return lax.ppermute(x, "cp", pairs)


def swapped(x):
    return lax.ppermute(x, "sec", [(0, 1), (1, 0)])


def local(
    prompt_states,
    prompt_queries,
    decode_states,
    decode_queries,
    latent_down,
    key_up,
    value_up,
    prompt_lengths,
    block_order,
    page_owner,
    decode_context,
):
    width = prompt_states.shape[-1]
    ci, sec = lax.axis_index("cp"), lax.axis_index("sec")
    own = jnp.dot(
        prompt_states.reshape(PPG * 2 * BLOCK, width), latent_down, preferred_element_type=jnp.float32
    )
    own = own.astype(jnp.bfloat16).reshape(UNITS, BLOCK, RANK)
    new = jnp.dot(
        decode_states.reshape(STEPS * ROW_GRP, width), latent_down, preferred_element_type=jnp.float32
    ).astype(jnp.bfloat16)
    meta, pages, limit = scalar_tables(
        block_order, prompt_lengths, decode_context, page_owner[0], ci, sec
    )
    qt, dqt = prepare_queries(prompt_queries, decode_queries, key_up)

    plane = jnp.stack([own, shifted(own, 0, -1), shifted(own, 0, 2), shifted(own, 0, 1)])
    new_far = swapped(new)
    up, down = shifted(plane, 1, 0), shifted(plane, -1, 0)
    plane_far = swapped(plane)
    state = attend_chunk(0, meta, [plane], [plane_far], qt, dqt, limit, new=(new, new_far))
    others = [(plane.reshape(YN, UNITS, BLOCK, RANK), plane_far)]
    for c in range(1, 4):
        if c < 3:
            up_next, down_next = shifted(up, 1, 0), shifted(down, -1, 0)
        else:
            up_next, down_next = shifted(up[:2], 1, 0), shifted(down[2:], -1, 0)
        up_far, down_far = swapped(up), swapped(down)
        others += [(up, up_far), (down, down_far)]
        state = attend_chunk(c, meta, [up, down], [up_far, down_far], qt, dqt, limit, state=state)
        up, down = up_next, down_next
    ending = dict(pages=pages, others=others, value_up=value_up)
    prefill_out, decode_out, cache = attend_chunk(
        4, meta, [up, down], [swapped(up), swapped(down)], qt, dqt, limit, state=state, ending=ending
    )
    return prefill_out, decode_out, cache.reshape(1, 1, PAGES_DEV * PAGE, 2 * RANK)


def solution(mesh):
    placed = (
        P("grp", "cp", None),
        P("grp", "cp", "sec"),
        P(None, "grp", None),
        P(None, "grp", "sec"),
        P(None, "sec"),
        P(None, "sec"),
        P(None, "sec"),
        P("grp"),
        P(),
        P("grp", None, None),
        P("grp"),
    )
    return jax.shard_map(
        local,
        mesh=mesh,
        in_specs=placed,
        out_specs=(P("grp", "cp", "sec"), P(None, "grp", "sec"), P("grp", "cp", None, None)),
        check_vma=False,
    )
```

```python
import functools
import math

import jax
import jax.numpy as jnp
import numpy as np
from jax import lax
from jax.experimental import pallas as pl
from jax.experimental.pallas import tpu as pltpu
from jax.sharding import PartitionSpec as P


HEAD = 128
RANK = 128
HEADS = 4
BLOCK = 96
PAGE = 16
PPG = 2
ROW_GRP = 32
HALF_GRP = ROW_GRP // PPG
STEPS = 3
PAGES_DEV = 24
ZN, YN = 8, 4
CP = ZN * YN
UNITS = 4
QL = HEADS * BLOCK
DH = 64
DL = HEADS * DH
G = 4
GK = G * BLOCK
NEG = -1e30
SCALE2 = math.log2(math.e) / math.sqrt(HEAD)

CHUNK_Z = [[0], [7, 1], [6, 2], [5, 3], [4]]
SLOT_Z = np.zeros((5, 16), np.int32)
SLOT_Y = np.zeros((5, 16), np.int32)
SLOT_A = np.zeros((5, 16), np.int32)
SLOT_ROW = np.zeros((5, 16), np.int32)
SLOT_OK = np.zeros((5, 16), bool)
for _c, _zs in enumerate(CHUNK_Z):
    for _i, _dz in enumerate(_zs):
        for _dy in range(YN):
            for _a in range(2):
                _j = _i * 8 + _dy * 2 + _a
                SLOT_Z[_c, _j], SLOT_Y[_c, _j], SLOT_A[_c, _j] = _dz, _dy, _a
                SLOT_ROW[_c, _j] = _i * 16 + _dy * 4 + _a
                SLOT_OK[_c, _j] = True

M_IDX, M_ORD, M_ALL, M_DEC, M_OWN, M_LEN, M_POS = 0, 16, 34, 36, 37, 39, 41
PG_HAS, PG_K, PG_SLOT = 0, 1, 2


def lookup(table, indices):
    matches = indices[..., None] == jnp.arange(table.shape[0], dtype=jnp.int32)
    return jnp.sum(jnp.where(matches, table, 0), axis=-1)


def scalar_tables(block_order, lengths, contexts, owners, ci, sec):
    z, y = ci // YN, ci % YN
    source = ((z + SLOT_Z) % ZN) * YN + (y + SLOT_Y) % YN
    order = lookup(block_order, 2 * source + SLOT_A)
    order = jnp.where(SLOT_OK, order, 4096 + np.arange(16, dtype=np.int32))
    rank = jnp.sum((order[:, None, :] < order[:, :, None]).astype(jnp.int32), axis=-1)
    place = rank[:, None, :] == np.arange(16, dtype=np.int32)[None, :, None]
    idx = jnp.sum(jnp.where(place, SLOT_ROW[:, None, :], 0), axis=-1)
    ranked = jnp.sum(jnp.where(place, order[:, None, :], 0), axis=-1)
    own = lookup(block_order, 2 * ci + np.arange(2, dtype=np.int32))
    alive = own * BLOCK < jnp.max(lengths)
    strict = jnp.sum((order[:, None, :] < own[None, :, None]) & alive[None, :, None], axis=-1)
    every = jnp.sum((order[:, None, :] <= own[None, :, None]) & alive[None, :, None], axis=-1)
    row_prompt = np.arange(ROW_GRP, dtype=np.int32) // HALF_GRP
    limits = jnp.minimum(contexts, jnp.where(row_prompt == 0, lengths[0], lengths[1]))
    dec = jnp.sum(order * BLOCK < jnp.max(limits), axis=-1, keepdims=True)
    spread = jnp.broadcast_to(
        jnp.concatenate([own, lengths, jnp.stack([z, y, sec])])[None], (5, 7)
    )
    meta = jnp.concatenate(
        [idx, ranked, strict.astype(jnp.int32), every.astype(jnp.int32), dec.astype(jnp.int32), spread],
        axis=1,
    ).astype(jnp.int32)
    mine = owners == ci
    has = jnp.sum(mine.astype(jnp.int32), axis=1)
    page = jnp.sum(jnp.where(mine, np.arange(PAGES_DEV, dtype=np.int32), 0), axis=1)
    before = np.arange(CP)[None, :] < np.arange(CP)[:, None]
    slot = jnp.sum(jnp.where(before, has[None, :], 0), axis=1)
    pages = jnp.stack([has, page, slot]).astype(jnp.int32)
    limit_rows = limits.reshape(PPG, 1, 1, HALF_GRP)
    limit_lanes = jnp.broadcast_to(limit_rows, (PPG, HEADS, STEPS, HALF_GRP)).reshape(PPG, HEADS, 48)
    limit_lanes = jnp.pad(limit_lanes, ((0, 0), (0, 0), (0, DH - 48))).reshape(PPG, 1, DL)
    return meta, pages, limit_lanes


def queries_kernel(q_ref, dq_ref, u_ref, qt_ref, dqt_ref):
    for p in range(PPG):
        for a in range(2):
            rows = []
            for h in range(HEADS):
                cols = slice(h * HEAD, (h + 1) * HEAD)
                rows.append(
                    lax.dot_general(
                        q_ref[p, a * BLOCK : (a + 1) * BLOCK, cols],
                        u_ref[:, cols],
                        (((1,), (1,)), ((), ())),
                        preferred_element_type=jnp.float32,
                    )
                )
            qt_ref[p * 2 + a] = jnp.concatenate(rows, axis=0).T.astype(jnp.bfloat16)
        rows = []
        for h in range(HEADS):
            cols = slice(h * HEAD, (h + 1) * HEAD)
            q = jnp.concatenate(
                [dq_ref[t, p * HALF_GRP : (p + 1) * HALF_GRP, cols] for t in range(STEPS)]
                + [jnp.zeros((HALF_GRP, HEAD), jnp.bfloat16)],
                axis=0,
            )
            rows.append(
                lax.dot_general(
                    q, u_ref[:, cols], (((1,), (1,)), ((), ())), preferred_element_type=jnp.float32
                )
            )
        dqt_ref[p] = jnp.concatenate(rows, axis=0).T.astype(jnp.bfloat16)


def prepare_queries(prompt_queries, decode_queries, key_up):
    return pl.pallas_call(
        queries_kernel,
        out_shape=(
            jax.ShapeDtypeStruct((UNITS, RANK, QL), jnp.bfloat16),
            jax.ShapeDtypeStruct((PPG, RANK, DL), jnp.bfloat16),
        ),
        cost_estimate=pl.CostEstimate(flops=10**9, bytes_accessed=10**6, transcendentals=0),
        name="queries",
    )(prompt_queries, decode_queries, key_up)


def softmax_step(s, keep, v, m_ref, l_ref, acc_ref, at):
    s = jnp.where(keep, s * SCALE2, NEG)
    old = m_ref[at]
    new = jnp.maximum(old, jnp.max(s, axis=0, keepdims=True))
    factor = jnp.exp2(old - new)
    w = jnp.exp2(s - new)
    m_ref[at] = new
    l_ref[at] = l_ref[at] * factor + jnp.sum(w, axis=0, keepdims=True)
    w = w.astype(jnp.bfloat16)

    def weigh():
        part = lax.dot_general(v, w, (((0,), (0,)), ((), ())), preferred_element_type=jnp.float32)
        acc_ref[at] = acc_ref[at] * factor + part

    return weigh


def chunk_kernel(chunk, n_src, sizes, first, last, *refs):
    refs = list(refs)
    meta = refs.pop(0)
    pages = refs.pop(0) if last else None
    mine = [refs.pop(0) for _ in range(n_src)]
    theirs = [refs.pop(0) for _ in range(n_src)]
    qt, dqt, limit = refs.pop(0), refs.pop(0), refs.pop(0)
    if first:
        new_mine, new_theirs = refs.pop(0), refs.pop(0)
    else:
        state_in = [refs.pop(0) for _ in range(6)]
    if last:
        others = [(refs.pop(0), refs.pop(0)) for _ in range(7)]
        vup = refs.pop(0)
        out_ref, dec_ref, cache_ref = refs.pop(0), refs.pop(0), refs.pop(0)
    else:
        state_out = [refs.pop(0) for _ in range(6)]
    kbuf, vbuf, sbuf, dsbuf, offset, sems = [refs.pop(0) for _ in range(6)]
    if last:
        page_sems = refs.pop(0)
        state = state_in
    else:
        state = state_out
    m, l, acc, dm, dl, dacc = state

    sec = meta[chunk, M_POS + 2]
    spans, at = [], 0
    for n in sizes:
        spans.append((at, n))
        at += n

    def copies(k_src, v_src):
        made = []
        for i, (start, n) in enumerate(spans):
            made.append(pltpu.make_async_copy(k_src[i], kbuf.at[pl.ds(start, n)], sems.at[2 * i]))
            made.append(pltpu.make_async_copy(v_src[i], vbuf.at[pl.ds(start, n)], sems.at[2 * i + 1]))
        return made

    @pl.when(sec == 0)
    def _():
        for copy in copies(mine, theirs):
            copy.start()

    @pl.when(sec != 0)
    def _():
        for copy in copies(theirs, mine):
            copy.start()

    if last:
        z, y = meta[chunk, M_POS], meta[chunk, M_POS + 1]
        table = [(0, dy, others[0][0].at[dy], others[0][1].at[dy]) for dy in range(YN)]
        for i, dz in enumerate([7, 1, 6, 2, 5, 3]):
            table += [(dz, dy, others[1 + i][0].at[dy], others[1 + i][1].at[dy]) for dy in range(YN)]
        for i in range(2):
            table += [(4, 2 * i + e, mine[i].at[pl.ds(e * 4, 4)], theirs[i].at[pl.ds(e * 4, 4)]) for e in range(2)]

        def page_copies(n, dz, dy, own_src, far_src):
            s = lax.rem(z + dz, ZN) * YN + lax.rem(y + dy, YN)
            page, slot = pages[PG_K, s], pages[PG_SLOT, s]
            block, row = page // 6, pl.multiple_of(lax.rem(page, 6) * PAGE, PAGE)
            rows = pl.ds(pl.multiple_of(jnp.minimum(slot, PAGES_DEV - 1) * PAGE, PAGE), PAGE)
            own_at, far_at = sec * RANK, (1 - sec) * RANK
            return (
                pages[PG_HAS, s] > 0,
                pltpu.make_async_copy(
                    own_src.at[block, pl.ds(row, PAGE), :],
                    cache_ref.at[rows, pl.ds(pl.multiple_of(own_at, RANK), RANK)],
                    page_sems.at[2 * n],
                ),
                pltpu.make_async_copy(
                    far_src.at[block, pl.ds(row, PAGE), :],
                    cache_ref.at[rows, pl.ds(pl.multiple_of(far_at, RANK), RANK)],
                    page_sems.at[2 * n + 1],
                ),
            )

        for n, entry in enumerate(table):
            has, one, two = page_copies(n, *entry)

            @pl.when(has)
            def _(one=one, two=two):
                one.start()
                two.start()

    if first:
        m[...] = jnp.full(m.shape, NEG, jnp.float32)
        l[...] = jnp.zeros(l.shape, jnp.float32)
        acc[...] = jnp.zeros(acc.shape, jnp.float32)
        is_key = sec == 0
        lane = lax.broadcasted_iota(jnp.int32, (1, DL), 1)
        step_of = lax.rem(lane, DH) // HALF_GRP
        for p in range(PPG):
            scores, values = [], []
            for t in range(STEPS):
                rows = slice(t * ROW_GRP + p * HALF_GRP, t * ROW_GRP + (p + 1) * HALF_GRP)
                a, b = new_mine[rows, :].astype(jnp.float32), new_theirs[rows, :].astype(jnp.float32)
                k, v = jnp.where(is_key, a, b), jnp.where(is_key, b, a)
                k = jnp.concatenate([k] * (DL // HALF_GRP), axis=0).T
                values.append(jnp.concatenate([v] * (DL // HALF_GRP), axis=0).T)
                s = jnp.sum(dqt[p].astype(jnp.float32) * k, axis=0, keepdims=True) * SCALE2
                scores.append(jnp.where(t <= step_of, s, NEG))
            peak = jnp.maximum(jnp.maximum(scores[0], scores[1]), scores[2])
            weights = [jnp.exp2(s - peak) for s in scores]
            dm[p] = peak
            dl[p] = weights[0] + weights[1] + weights[2]
            total = jnp.zeros((RANK, DL), jnp.float32)
            for w, v in zip(weights, values):
                total = total + w.astype(jnp.bfloat16).astype(jnp.float32) * v
            dacc[p] = total
    elif not last:
        for src, dst in zip(state_in, state_out):
            dst[...] = src[...]

    for copy in copies(mine, theirs):
        copy.wait()

    def rows_of(buf, g, p):
        return jnp.concatenate([buf[meta[chunk, M_IDX + g * G + j] + 2 * p] for j in range(G)], axis=0)

    key_row = lax.broadcasted_iota(jnp.int32, (BLOCK, QL), 0)
    query_row = lax.rem(lax.broadcasted_iota(jnp.int32, (BLOCK, QL), 1), BLOCK)
    offset[...] = key_row - query_row
    groups = [(meta[chunk, M_ALL + a] + G - 1) // G for a in range(2)]
    work = groups[0] + groups[1]

    def part_of(w):
        a = jnp.where(w >= groups[0], 1, 0)
        return a, w - a * groups[0]

    def scores(w, p):
        a, g = part_of(w)
        sbuf[p] = jnp.dot(rows_of(kbuf, g, p), qt[2 * p + a], preferred_element_type=jnp.float32)

    @pl.when(work > 0)
    def _():
        for p in range(PPG):
            scores(0, p)

    def step(w, carry):
        a, g = part_of(w)
        own = meta[chunk, M_OWN + a]
        keep = jnp.concatenate(
            [offset[...] <= (own - meta[chunk, M_ORD + g * G + j]) * BLOCK for j in range(G)], axis=0
        )
        after = jnp.minimum(w + 1, work - 1)
        for p in range(PPG):
            weigh = softmax_step(sbuf[p], keep, rows_of(vbuf, g, p), m, l, acc, 2 * p + a)
            scores(after, p)
            weigh()
        return carry

    lax.fori_loop(0, work, step, 0)

    dec_row = lax.broadcasted_iota(jnp.int32, (BLOCK, DL), 0)
    dec_work = (meta[chunk, M_DEC] + G - 1) // G

    def dec_scores(g, p):
        dsbuf[p] = jnp.dot(rows_of(kbuf, g, p), dqt[p], preferred_element_type=jnp.float32)

    @pl.when(dec_work > 0)
    def _():
        for p in range(PPG):
            dec_scores(0, p)

    def dec_step(g, carry):
        after = jnp.minimum(g + 1, dec_work - 1)
        for p in range(PPG):
            keep = jnp.concatenate(
                [dec_row < limit[p] - meta[chunk, M_ORD + g * G + j] * BLOCK for j in range(G)], axis=0
            )
            weigh = softmax_step(dsbuf[p], keep, rows_of(vbuf, g, p), dm, dl, dacc, p)
            dec_scores(after, p)
            weigh()
        return carry

    lax.fori_loop(0, dec_work, dec_step, 0)

    if last:
        row = lax.broadcasted_iota(jnp.int32, (BLOCK, HEAD), 0)
        for p in range(PPG):
            for a in range(2):
                at = p * 2 + a
                o = (acc[at] / l[at]).T.astype(jnp.bfloat16)
                live = row + meta[chunk, M_OWN + a] * BLOCK < meta[chunk, M_LEN + p]
                for h in range(HEADS):
                    cols = slice(h * HEAD, (h + 1) * HEAD)
                    r = jnp.dot(
                        o[h * BLOCK : (h + 1) * BLOCK], vup[:, cols], preferred_element_type=jnp.float32
                    )
                    out_ref[p, a * BLOCK : (a + 1) * BLOCK, cols] = jnp.where(live, r, 0.0).astype(
                        jnp.bfloat16
                    )
            o = (dacc[p] / dl[p]).T.astype(jnp.bfloat16)
            for h in range(HEADS):
                cols = slice(h * HEAD, (h + 1) * HEAD)
                r = jnp.dot(
                    o[h * DH : (h + 1) * DH], vup[:, cols], preferred_element_type=jnp.float32
                ).astype(jnp.bfloat16)
                for t in range(STEPS):
                    dec_ref[t, p * HALF_GRP : (p + 1) * HALF_GRP, cols] = r[t * HALF_GRP : (t + 1) * HALF_GRP]
        for n, entry in enumerate(table):
            has, one, two = page_copies(n, *entry)

            @pl.when(has)
            def _(one=one, two=two):
                one.wait()
                two.wait()


STATE = (
    jax.ShapeDtypeStruct((UNITS, 1, QL), jnp.float32),
    jax.ShapeDtypeStruct((UNITS, 1, QL), jnp.float32),
    jax.ShapeDtypeStruct((UNITS, RANK, QL), jnp.float32),
    jax.ShapeDtypeStruct((PPG, 1, DL), jnp.float32),
    jax.ShapeDtypeStruct((PPG, 1, DL), jnp.float32),
    jax.ShapeDtypeStruct((PPG, RANK, DL), jnp.float32),
)


def attend_chunk(chunk, meta, mine, theirs, qt, dqt, limit, state=None, new=None, ending=None):
    first, last = state is None, ending is not None
    smem, vmem = pl.BlockSpec(memory_space=pltpu.SMEM), pl.BlockSpec(memory_space=pltpu.VMEM)
    anywhere = pl.BlockSpec(memory_space=pl.ANY)
    sizes = [a.size // (BLOCK * RANK) for a in mine]
    flat = [a.reshape(-1, BLOCK, RANK) for a in [*mine, *theirs]]
    args, specs = [meta], [smem]
    if last:
        args, specs = args + [ending["pages"]], specs + [smem]
    args, specs = args + flat, specs + [anywhere] * len(flat)
    args, specs = args + [qt, dqt, limit], specs + [vmem] * 3
    if first:
        args, specs = args + list(new), specs + [vmem] * 2
    else:
        args, specs = args + list(state), specs + [vmem] * 6
    rows = sum(sizes)
    scratch = [
        pltpu.VMEM((rows, BLOCK, RANK), jnp.bfloat16),
        pltpu.VMEM((rows, BLOCK, RANK), jnp.bfloat16),
        pltpu.VMEM((PPG, GK, QL), jnp.float32),
        pltpu.VMEM((PPG, GK, DL), jnp.float32),
        pltpu.VMEM((BLOCK, QL), jnp.int32),
        pltpu.SemaphoreType.DMA((2 * len(mine),)),
    ]
    if last:
        for pair in ending["others"]:
            args, specs = args + list(pair), specs + [anywhere] * 2
        args, specs = args + [ending["value_up"]], specs + [vmem]
        shapes = (
            jax.ShapeDtypeStruct((PPG, 2 * BLOCK, HEADS * HEAD), jnp.bfloat16),
            jax.ShapeDtypeStruct((STEPS, ROW_GRP, HEADS * HEAD), jnp.bfloat16),
            jax.ShapeDtypeStruct((PAGES_DEV * PAGE, 2 * RANK), jnp.bfloat16),
        )
        scratch.append(pltpu.SemaphoreType.DMA((2 * CP,)))
    else:
        shapes = STATE
    work = rows * BLOCK * (2 * QL + DL) * RANK * 4
    return pl.pallas_call(
        functools.partial(chunk_kernel, chunk, len(mine), sizes, first, last),
        out_shape=shapes,
        in_specs=specs,
        out_specs=[vmem] * len(shapes),
        scratch_shapes=scratch,
        cost_estimate=pl.CostEstimate(flops=2 * work, bytes_accessed=4 * 10**6, transcendentals=work // 512),
        compiler_params=pltpu.CompilerParams(vmem_limit_bytes=48 * 2**20),
    )(*args)


def shifted(x, dz, dy):
    pairs = [
        (z * YN + y, ((z + dz) % ZN) * YN + (y + dy) % YN) for z in range(ZN) for y in range(YN)
    ]
    return lax.ppermute(x, "cp", pairs)


def swapped(x):
    return lax.ppermute(x, "sec", [(0, 1), (1, 0)])


def body(
    prompt_states,
    prompt_queries,
    decode_states,
    decode_queries,
    latent_down,
    key_up,
    value_up,
    prompt_lengths,
    block_order,
    page_owner,
    decode_context,
):
    width = prompt_states.shape[-1]
    ci, sec = lax.axis_index("cp"), lax.axis_index("sec")
    own = jnp.dot(
        prompt_states.reshape(PPG * 2 * BLOCK, width), latent_down, preferred_element_type=jnp.float32
    )
    own = own.astype(jnp.bfloat16).reshape(UNITS, BLOCK, RANK)
    new = jnp.dot(
        decode_states.reshape(STEPS * ROW_GRP, width), latent_down, preferred_element_type=jnp.float32
    ).astype(jnp.bfloat16)
    meta, pages, limit = scalar_tables(
        block_order, prompt_lengths, decode_context, page_owner[0], ci, sec
    )
    qt, dqt = prepare_queries(prompt_queries, decode_queries, key_up)

    plane = jnp.stack([own, shifted(own, 0, -1), shifted(own, 0, 2), shifted(own, 0, 1)])
    new_far = swapped(new)
    up, down = shifted(plane, 1, 0), shifted(plane, -1, 0)
    plane_far = swapped(plane)
    state = attend_chunk(0, meta, [plane], [plane_far], qt, dqt, limit, new=(new, new_far))
    others = [(plane, plane_far)]
    for c in range(1, 4):
        if c < 3:
            up_next = shifted(up, 1, 0)
            down_next = shifted(down, -1, 0)
        else:
            up_next = shifted(up[:2], 1, 0)
            down_next = shifted(down[2:], -1, 0)
        up_far, down_far = swapped(up), swapped(down)
        others += [(up, up_far), (down, down_far)]
        state = attend_chunk(c, meta, [up, down], [up_far, down_far], qt, dqt, limit, state=state)
        up, down = up_next, down_next
    ending = dict(pages=pages, others=others, value_up=value_up)
    far = [swapped(up), swapped(down)]
    prefill_out, decode_out, cache = attend_chunk(4, meta, [up, down], far, qt, dqt, limit, state=state, ending=ending)
    return prefill_out, decode_out, cache.reshape(1, 1, PAGES_DEV * PAGE, 2 * RANK)


def solution(mesh):
    placed = (
        P("grp", "cp", None),
        P("grp", "cp", "sec"),
        P(None, "grp", None),
        P(None, "grp", "sec"),
        P(None, "sec"),
        P(None, "sec"),
        P(None, "sec"),
        P("grp"),
        P(),
        P("grp", None, None),
        P("grp"),
    )
    return jax.shard_map(
        body,
        mesh=mesh,
        in_specs=placed,
        out_specs=(P("grp", "cp", "sec"), P(None, "grp", "sec"), P("grp", "cp", None, None)),
        check_vma=False,
    )
```

```python
import functools
import math

import jax
import jax.numpy as jnp
import numpy as np
from jax import lax
from jax.experimental import pallas as pl
from jax.experimental.pallas import tpu as pltpu
from jax.sharding import PartitionSpec as P


HEAD = 128
RANK = 128
HEADS = 4
BLOCK = 96
PAGE = 16
PPG = 2
ROW_GRP = 32
HALF_GRP = ROW_GRP // PPG
STEPS = 3
PAGES_DEV = 24
ZN, YN = 8, 4
CP = ZN * YN
UNITS = 4
QL = HEADS * BLOCK
DH = 64
DL = HEADS * DH
G = 4
GK = G * BLOCK
NEG = -1e30
SCALE2 = math.log2(math.e) / math.sqrt(HEAD)

CHUNK_Z = [[0], [7, 1], [6, 2], [5, 3], [4]]
SLOT_Z = np.zeros((5, 16), np.int32)
SLOT_Y = np.zeros((5, 16), np.int32)
SLOT_A = np.zeros((5, 16), np.int32)
SLOT_ROW = np.zeros((5, 16), np.int32)
SLOT_OK = np.zeros((5, 16), bool)
for _c, _zs in enumerate(CHUNK_Z):
    for _i, _dz in enumerate(_zs):
        for _dy in range(YN):
            for _a in range(2):
                _j = _i * 8 + _dy * 2 + _a
                SLOT_Z[_c, _j], SLOT_Y[_c, _j], SLOT_A[_c, _j] = _dz, _dy, _a
                SLOT_ROW[_c, _j] = _i * 16 + _dy * 4 + _a
                SLOT_OK[_c, _j] = True

PG_HAS, PG_K, PG_SLOT = 0, 1, 2


def lookup(table, indices):
    matches = indices[..., None] == jnp.arange(table.shape[0], dtype=jnp.int32)
    return jnp.sum(jnp.where(matches, table, 0), axis=-1)


def page_table(owners, ci):
    mine = owners == ci
    has = jnp.sum(mine.astype(jnp.int32), axis=1)
    page = jnp.sum(jnp.where(mine, np.arange(PAGES_DEV, dtype=np.int32), 0), axis=1)
    before = np.arange(CP)[None, :] < np.arange(CP)[:, None]
    slot = jnp.sum(jnp.where(before, has[None, :], 0), axis=1)
    return jnp.stack([has, page, slot]).astype(jnp.int32)


def lane_limits(contexts, lengths):
    lane = np.arange(DL, dtype=np.int32)
    row = np.arange(PPG, dtype=np.int32)[:, None] * HALF_GRP + lane % HALF_GRP
    spare = (lane % DH >= STEPS * HALF_GRP)[None, :]
    prompt = np.broadcast_to(np.arange(PPG, dtype=np.int32)[:, None], (PPG, DL))
    limits = jnp.minimum(lookup(contexts, row), lookup(lengths, prompt))
    return jnp.where(spare, 0, limits).reshape(PPG, 1, DL)


def absorb_queries(q_ref, dq_ref, u_ref, qt_ref, dqt_ref):
    for p in range(PPG):
        for a in range(2):
            rows = []
            for h in range(HEADS):
                cols = slice(h * HEAD, (h + 1) * HEAD)
                rows.append(
                    lax.dot_general(
                        q_ref[p, a * BLOCK : (a + 1) * BLOCK, cols],
                        u_ref[:, cols],
                        (((1,), (1,)), ((), ())),
                        preferred_element_type=jnp.float32,
                    )
                )
            qt_ref[p * 2 + a] = jnp.concatenate(rows, axis=0).T.astype(jnp.bfloat16)
        rows = []
        for h in range(HEADS):
            cols = slice(h * HEAD, (h + 1) * HEAD)
            q = jnp.concatenate(
                [dq_ref[t, p * HALF_GRP : (p + 1) * HALF_GRP, cols] for t in range(STEPS)]
                + [jnp.zeros((HALF_GRP, HEAD), jnp.bfloat16)],
                axis=0,
            )
            rows.append(
                lax.dot_general(
                    q, u_ref[:, cols], (((1,), (1,)), ((), ())), preferred_element_type=jnp.float32
                )
            )
        dqt_ref[p] = jnp.concatenate(rows, axis=0).T.astype(jnp.bfloat16)


def take_scores(k, q, keep_of, s_ref, peak_ref, p):
    s = jnp.dot(k, q, preferred_element_type=jnp.float32)
    peak = None
    for j in range(G):
        rows = slice(j * BLOCK, (j + 1) * BLOCK)
        part = jnp.where(keep_of(j), s[rows], NEG)
        s_ref[p, rows] = part
        top = jnp.max(part, axis=0, keepdims=True)
        peak = top if peak is None else jnp.maximum(peak, top)
    peak_ref[p] = peak


def weights_of(s_ref, peak_ref, p, m_ref, l_ref, at):
    old = m_ref[at]
    new = jnp.maximum(old, peak_ref[p] * SCALE2)
    factor = jnp.exp2(old - new)
    total = l_ref[at] * factor
    parts = []
    for j in range(G):
        w = jnp.exp2(s_ref[p, j * BLOCK : (j + 1) * BLOCK] * SCALE2 - new)
        total = total + jnp.sum(w, axis=0, keepdims=True)
        parts.append(w.astype(jnp.bfloat16))
    m_ref[at] = new
    l_ref[at] = total
    return jnp.concatenate(parts, axis=0), factor


def weigh(v, w, factor, acc_ref, at):
    part = lax.dot_general(v, w, (((0,), (0,)), ((), ())), preferred_element_type=jnp.float32)
    acc_ref[at] = acc_ref[at] * factor + part


def chunk_kernel(chunk, n_src, sizes, first, last, *refs):
    refs = list(refs)
    order, lengths, contexts = refs.pop(0), refs.pop(0), refs.pop(0)
    pages = refs.pop(0) if last else None
    mine = [refs.pop(0) for _ in range(n_src)]
    theirs = [refs.pop(0) for _ in range(n_src)]
    limit = refs.pop(0)
    if first:
        new_mine, new_theirs, q_in, dq_in, key_up = [refs.pop(0) for _ in range(5)]
    else:
        qt, dqt = refs.pop(0), refs.pop(0)
        state_in = [refs.pop(0) for _ in range(6)]
    if last:
        others = [(refs.pop(0), refs.pop(0)) for _ in range(7)]
        vup = refs.pop(0)
        out_ref, dec_ref, cache_ref = refs.pop(0), refs.pop(0), refs.pop(0)
    else:
        state_out = [refs.pop(0) for _ in range(6)]
        if first:
            qt, dqt = refs.pop(0), refs.pop(0)
    kbuf, vbuf, sbuf, dsbuf, peak, dpeak, offset, place, sems = [refs.pop(0) for _ in range(9)]
    if last:
        page_sems = refs.pop(0)
        state = state_in
    else:
        state = state_out
    m, l, acc, dm, dl, dacc = state

    sec, ci = lax.axis_index("sec"), lax.axis_index("cp")
    z, y = ci // YN, lax.rem(ci, YN)
    spans, at = [], 0
    for n in sizes:
        spans.append((at, n))
        at += n

    def copies(k_src, v_src):
        made = []
        for i, (start, n) in enumerate(spans):
            made.append(pltpu.make_async_copy(k_src[i], kbuf.at[pl.ds(start, n)], sems.at[2 * i]))
            made.append(pltpu.make_async_copy(v_src[i], vbuf.at[pl.ds(start, n)], sems.at[2 * i + 1]))
        return made

    @pl.when(sec == 0)
    def _():
        for copy in copies(mine, theirs):
            copy.start()

    @pl.when(sec != 0)
    def _():
        for copy in copies(theirs, mine):
            copy.start()

    if last:
        table = [(0, dy, others[0][0].at[dy], others[0][1].at[dy]) for dy in range(YN)]
        for i, dz in enumerate([7, 1, 6, 2, 5, 3]):
            table += [(dz, dy, others[1 + i][0].at[dy], others[1 + i][1].at[dy]) for dy in range(YN)]
        for i in range(2):
            table += [(4, 2 * i + e, mine[i].at[pl.ds(e * 4, 4)], theirs[i].at[pl.ds(e * 4, 4)]) for e in range(2)]

        def page_copies(n, dz, dy, own_src, far_src):
            s = lax.rem(z + dz, ZN) * YN + lax.rem(y + dy, YN)
            page, slot = pages[PG_K, s], pages[PG_SLOT, s]
            block, row = page // 6, pl.multiple_of(lax.rem(page, 6) * PAGE, PAGE)
            rows = pl.ds(pl.multiple_of(jnp.minimum(slot, PAGES_DEV - 1) * PAGE, PAGE), PAGE)
            own_at, far_at = sec * RANK, (1 - sec) * RANK
            return (
                pages[PG_HAS, s] > 0,
                pltpu.make_async_copy(
                    own_src.at[block, pl.ds(row, PAGE), :],
                    cache_ref.at[rows, pl.ds(pl.multiple_of(own_at, RANK), RANK)],
                    page_sems.at[2 * n],
                ),
                pltpu.make_async_copy(
                    far_src.at[block, pl.ds(row, PAGE), :],
                    cache_ref.at[rows, pl.ds(pl.multiple_of(far_at, RANK), RANK)],
                    page_sems.at[2 * n + 1],
                ),
            )

        for n, entry in enumerate(table):
            has, one, two = page_copies(n, *entry)

            @pl.when(has)
            def _(one=one, two=two):
                one.start()
                two.start()

    slots = [j for j in range(16) if SLOT_OK[chunk, j]]
    orders = []
    for j in slots:
        source = lax.rem(z + int(SLOT_Z[chunk, j]), ZN) * YN + lax.rem(y + int(SLOT_Y[chunk, j]), YN)
        orders.append(order[2 * source + int(SLOT_A[chunk, j])])
    ranks = [jnp.int32(0)] * len(slots)
    for i in range(len(slots)):
        for j in range(i):
            ahead = jnp.where(orders[j] < orders[i], 1, 0)
            ranks[i], ranks[j] = ranks[i] + ahead, ranks[j] + 1 - ahead
    for i, j in enumerate(slots):
        place[ranks[i]] = jnp.int32(int(SLOT_ROW[chunk, j]))
        place[16 + ranks[i]] = orders[i]
    owns = [order[2 * ci + a] for a in range(2)]
    longest = jnp.maximum(lengths[0], lengths[1])
    reach = jnp.int32(0)
    for n in range(ROW_GRP):
        reach = jnp.maximum(reach, jnp.minimum(contexts[n], lengths[n // HALF_GRP]))
    every = []
    for a in range(2):
        count = jnp.int32(0)
        for one in orders:
            count = count + jnp.where(one <= owns[a], 1, 0)
        every.append(jnp.where(owns[a] * BLOCK < longest, count, 0))
    dec_count = jnp.int32(0)
    for one in orders:
        dec_count = dec_count + jnp.where(one * BLOCK < reach, 1, 0)

    if first:
        absorb_queries(q_in, dq_in, key_up, qt, dqt)
        m[...] = jnp.full(m.shape, NEG, jnp.float32)
        l[...] = jnp.zeros(l.shape, jnp.float32)
        acc[...] = jnp.zeros(acc.shape, jnp.float32)
        is_key = sec == 0
        lane = lax.broadcasted_iota(jnp.int32, (1, DL), 1)
        step_of = lax.rem(lane, DH) // HALF_GRP
        for p in range(PPG):
            scores, values = [], []
            for t in range(STEPS):
                rows = slice(t * ROW_GRP + p * HALF_GRP, t * ROW_GRP + (p + 1) * HALF_GRP)
                a, b = new_mine[rows, :].astype(jnp.float32), new_theirs[rows, :].astype(jnp.float32)
                k, v = jnp.where(is_key, a, b), jnp.where(is_key, b, a)
                k = jnp.concatenate([k] * (DL // HALF_GRP), axis=0).T
                values.append(jnp.concatenate([v] * (DL // HALF_GRP), axis=0).T)
                s = jnp.sum(dqt[p].astype(jnp.float32) * k, axis=0, keepdims=True) * SCALE2
                scores.append(jnp.where(t <= step_of, s, NEG))
            top = jnp.maximum(jnp.maximum(scores[0], scores[1]), scores[2])
            weights = [jnp.exp2(s - top) for s in scores]
            dm[p] = top
            dl[p] = weights[0] + weights[1] + weights[2]
            total = jnp.zeros((RANK, DL), jnp.float32)
            for w, v in zip(weights, values):
                total = total + w.astype(jnp.bfloat16).astype(jnp.float32) * v
            dacc[p] = total
    elif not last:
        for src, dst in zip(state_in, state_out):
            dst[...] = src[...]

    for copy in copies(mine, theirs):
        copy.wait()

    def rows_of(buf, g, p):
        return jnp.concatenate([buf[place[g * G + j] + 2 * p] for j in range(G)], axis=0)

    key_row = lax.broadcasted_iota(jnp.int32, (BLOCK, QL), 0)
    query_row = lax.rem(lax.broadcasted_iota(jnp.int32, (BLOCK, QL), 1), BLOCK)
    offset[...] = key_row - query_row
    groups = [(every[a] + G - 1) // G for a in range(2)]
    work = groups[0] + groups[1]

    def part_of(w):
        a = jnp.where(w >= groups[0], 1, 0)
        return a, w - a * groups[0]

    def scores(w, p):
        a, g = part_of(w)
        own = jnp.where(a == 0, owns[0], owns[1])

        def keep_of(j):
            return offset[...] <= (own - place[16 + g * G + j]) * BLOCK

        take_scores(rows_of(kbuf, g, p), qt[2 * p + a], keep_of, sbuf, peak, p)

    @pl.when(work > 0)
    def _():
        for p in range(PPG):
            scores(0, p)

    def step(w, carry):
        a, g = part_of(w)
        after = jnp.minimum(w + 1, work - 1)
        for p in range(PPG):
            weights, factor = weights_of(sbuf, peak, p, m, l, 2 * p + a)
            scores(after, p)
            weigh(rows_of(vbuf, g, p), weights, factor, acc, 2 * p + a)
        return carry

    lax.fori_loop(0, work, step, 0)

    dec_row = lax.broadcasted_iota(jnp.int32, (BLOCK, DL), 0)
    dec_work = (dec_count + G - 1) // G

    def dec_scores(g, p):
        def keep_of(j):
            return dec_row < limit[p] - place[16 + g * G + j] * BLOCK

        take_scores(rows_of(kbuf, g, p), dqt[p], keep_of, dsbuf, dpeak, p)

    @pl.when(dec_work > 0)
    def _():
        for p in range(PPG):
            dec_scores(0, p)

    def dec_step(g, carry):
        after = jnp.minimum(g + 1, dec_work - 1)
        for p in range(PPG):
            weights, factor = weights_of(dsbuf, dpeak, p, dm, dl, p)
            dec_scores(after, p)
            weigh(rows_of(vbuf, g, p), weights, factor, dacc, p)
        return carry

    lax.fori_loop(0, dec_work, dec_step, 0)

    if last:
        row = lax.broadcasted_iota(jnp.int32, (BLOCK, HEAD), 0)
        for p in range(PPG):
            for a in range(2):
                at = p * 2 + a
                o = (acc[at] * (1.0 / l[at])).T.astype(jnp.bfloat16)
                live = row + owns[a] * BLOCK < lengths[p]
                for h in range(HEADS):
                    cols = slice(h * HEAD, (h + 1) * HEAD)
                    r = jnp.dot(
                        o[h * BLOCK : (h + 1) * BLOCK], vup[:, cols], preferred_element_type=jnp.float32
                    )
                    out_ref[p, a * BLOCK : (a + 1) * BLOCK, cols] = jnp.where(live, r, 0.0).astype(
                        jnp.bfloat16
                    )
            o = (dacc[p] * (1.0 / dl[p])).T.astype(jnp.bfloat16)
            for h in range(HEADS):
                cols = slice(h * HEAD, (h + 1) * HEAD)
                r = jnp.dot(
                    o[h * DH : (h + 1) * DH], vup[:, cols], preferred_element_type=jnp.float32
                ).astype(jnp.bfloat16)
                for t in range(STEPS):
                    dec_ref[t, p * HALF_GRP : (p + 1) * HALF_GRP, cols] = r[t * HALF_GRP : (t + 1) * HALF_GRP]
        for n, entry in enumerate(table):
            has, one, two = page_copies(n, *entry)

            @pl.when(has)
            def _(one=one, two=two):
                one.wait()
                two.wait()


STATE = (
    jax.ShapeDtypeStruct((UNITS, 1, QL), jnp.float32),
    jax.ShapeDtypeStruct((UNITS, 1, QL), jnp.float32),
    jax.ShapeDtypeStruct((UNITS, RANK, QL), jnp.float32),
    jax.ShapeDtypeStruct((PPG, 1, DL), jnp.float32),
    jax.ShapeDtypeStruct((PPG, 1, DL), jnp.float32),
    jax.ShapeDtypeStruct((PPG, RANK, DL), jnp.float32),
)


QUERIES = (
    jax.ShapeDtypeStruct((UNITS, RANK, QL), jnp.bfloat16),
    jax.ShapeDtypeStruct((PPG, RANK, DL), jnp.bfloat16),
)


def attend_chunk(chunk, control, mine, theirs, limit, queries=None, state=None, start=None, ending=None):
    first, last = state is None, ending is not None
    smem, vmem = pl.BlockSpec(memory_space=pltpu.SMEM), pl.BlockSpec(memory_space=pltpu.VMEM)
    anywhere = pl.BlockSpec(memory_space=pl.ANY)
    sizes = [a.size // (BLOCK * RANK) for a in mine]
    flat = [a.reshape(-1, BLOCK, RANK) for a in [*mine, *theirs]]
    args, specs = list(control), [smem] * 3
    if last:
        args, specs = args + [ending["pages"]], specs + [smem]
    args, specs = args + flat, specs + [anywhere] * len(flat)
    args, specs = args + [limit], specs + [vmem]
    if first:
        args, specs = args + list(start), specs + [vmem] * 5
    else:
        args, specs = args + list(queries) + list(state), specs + [vmem] * 8
    rows = sum(sizes)
    scratch = [
        pltpu.VMEM((rows, BLOCK, RANK), jnp.bfloat16),
        pltpu.VMEM((rows, BLOCK, RANK), jnp.bfloat16),
        pltpu.VMEM((PPG, GK, QL), jnp.float32),
        pltpu.VMEM((PPG, GK, DL), jnp.float32),
        pltpu.VMEM((PPG, 1, QL), jnp.float32),
        pltpu.VMEM((PPG, 1, DL), jnp.float32),
        pltpu.VMEM((BLOCK, QL), jnp.int32),
        pltpu.SMEM((32,), jnp.int32),
        pltpu.SemaphoreType.DMA((2 * len(mine),)),
    ]
    if last:
        for pair in ending["others"]:
            args, specs = args + list(pair), specs + [anywhere] * 2
        args, specs = args + [ending["value_up"]], specs + [vmem]
        shapes = (
            jax.ShapeDtypeStruct((PPG, 2 * BLOCK, HEADS * HEAD), jnp.bfloat16),
            jax.ShapeDtypeStruct((STEPS, ROW_GRP, HEADS * HEAD), jnp.bfloat16),
            jax.ShapeDtypeStruct((PAGES_DEV * PAGE, 2 * RANK), jnp.bfloat16),
        )
        scratch.append(pltpu.SemaphoreType.DMA((2 * CP,)))
    else:
        shapes = STATE + QUERIES if first else STATE
    work = rows * BLOCK * (2 * QL + DL) * RANK * 4
    return pl.pallas_call(
        functools.partial(chunk_kernel, chunk, len(mine), sizes, first, last),
        out_shape=shapes,
        in_specs=specs,
        out_specs=[vmem] * len(shapes),
        scratch_shapes=scratch,
        cost_estimate=pl.CostEstimate(flops=2 * work, bytes_accessed=4 * 10**6, transcendentals=work // 512),
        compiler_params=pltpu.CompilerParams(vmem_limit_bytes=20 * 2**20),
    )(*args)


def shifted(x, dz, dy):
    pairs = [
        (z * YN + y, ((z + dz) % ZN) * YN + (y + dy) % YN) for z in range(ZN) for y in range(YN)
    ]
    return lax.ppermute(x, "cp", pairs)


def swapped(x):
    return lax.ppermute(x, "sec", [(0, 1), (1, 0)])


def body(
    prompt_states,
    prompt_queries,
    decode_states,
    decode_queries,
    latent_down,
    key_up,
    value_up,
    prompt_lengths,
    block_order,
    page_owner,
    decode_context,
):
    width = prompt_states.shape[-1]
    ci = lax.axis_index("cp")
    own = jnp.dot(
        prompt_states.reshape(PPG * 2 * BLOCK, width), latent_down, preferred_element_type=jnp.float32
    )
    own = own.astype(jnp.bfloat16).reshape(UNITS, BLOCK, RANK)
    new = jnp.dot(
        decode_states.reshape(STEPS * ROW_GRP, width), latent_down, preferred_element_type=jnp.float32
    ).astype(jnp.bfloat16)
    control = (block_order, prompt_lengths, decode_context)
    pages = page_table(page_owner[0], ci)
    limit = lane_limits(decode_context, prompt_lengths)

    plane = jnp.stack([own, shifted(own, 0, -1), shifted(own, 0, 2), shifted(own, 0, 1)])
    new_far = swapped(new)
    up, down = shifted(plane, 1, 0), shifted(plane, -1, 0)
    plane_far = swapped(plane)
    start = (new, new_far, prompt_queries, decode_queries, key_up)
    *state, qt, dqt = attend_chunk(0, control, [plane], [plane_far], limit, start=start)
    others = [(plane, plane_far)]
    for c in range(1, 4):
        if c < 3:
            up_next = shifted(up, 1, 0)
            down_next = shifted(down, -1, 0)
        else:
            up_next = shifted(up[:2], 1, 0)
            down_next = shifted(down[2:], -1, 0)
        up_far, down_far = swapped(up), swapped(down)
        others += [(up, up_far), (down, down_far)]
        state = attend_chunk(
            c, control, [up, down], [up_far, down_far], limit, queries=(qt, dqt), state=state
        )
        up, down = up_next, down_next
    ending = dict(pages=pages, others=others, value_up=value_up)
    far = [swapped(up), swapped(down)]
    prefill_out, decode_out, cache = attend_chunk(
        4, control, [up, down], far, limit, queries=(qt, dqt), state=state, ending=ending
    )
    return prefill_out, decode_out, cache.reshape(1, 1, PAGES_DEV * PAGE, 2 * RANK)


def solution(mesh):
    placed = (
        P("grp", "cp", None),
        P("grp", "cp", "sec"),
        P(None, "grp", None),
        P(None, "grp", "sec"),
        P(None, "sec"),
        P(None, "sec"),
        P(None, "sec"),
        P("grp"),
        P(),
        P("grp", None, None),
        P("grp"),
    )
    return jax.shard_map(
        body,
        mesh=mesh,
        in_specs=placed,
        out_specs=(P("grp", "cp", "sec"), P(None, "grp", "sec"), P("grp", "cp", None, None)),
        check_vma=False,
    )
```

```python
import functools
import math

import jax
import jax.numpy as jnp
import numpy as np
from jax import lax
from jax.experimental import pallas as pl
from jax.experimental.pallas import tpu as pltpu
from jax.sharding import PartitionSpec as P


HEAD = 128
RANK = 128
HEADS = 4
BLOCK = 96
PAGE = 16
PPG = 2
ROW_GRP = 32
HALF_GRP = ROW_GRP // PPG
STEPS = 3
PAGES_DEV = 24
ZN, YN = 8, 4
CP = ZN * YN
UNITS = 4
QL = HEADS * BLOCK
DH = 64
DL = HEADS * DH
G = 4
GK = G * BLOCK
NEG = -1e30
SCALE2 = math.log2(math.e) / math.sqrt(HEAD)

CHUNK_Z = [[0], [7, 1], [6, 2], [5, 3], [4]]
SLOT_Z = np.zeros((5, 16), np.int32)
SLOT_Y = np.zeros((5, 16), np.int32)
SLOT_A = np.zeros((5, 16), np.int32)
SLOT_ROW = np.zeros((5, 16), np.int32)
SLOT_OK = np.zeros((5, 16), bool)
for _c, _zs in enumerate(CHUNK_Z):
    for _i, _dz in enumerate(_zs):
        for _dy in range(YN):
            for _a in range(2):
                _j = _i * 8 + _dy * 2 + _a
                SLOT_Z[_c, _j], SLOT_Y[_c, _j], SLOT_A[_c, _j] = _dz, _dy, _a
                SLOT_ROW[_c, _j] = _i * 16 + _dy * 4 + _a
                SLOT_OK[_c, _j] = True

PG_HAS, PG_K, PG_SLOT = 0, 1, 2


def lookup(table, indices):
    matches = indices[..., None] == jnp.arange(table.shape[0], dtype=jnp.int32)
    return jnp.sum(jnp.where(matches, table, 0), axis=-1)


def page_table(owners, ci):
    mine = owners == ci
    has = jnp.sum(mine.astype(jnp.int32), axis=1)
    page = jnp.sum(jnp.where(mine, np.arange(PAGES_DEV, dtype=np.int32), 0), axis=1)
    before = np.arange(CP)[None, :] < np.arange(CP)[:, None]
    slot = jnp.sum(jnp.where(before, has[None, :], 0), axis=1)
    return jnp.stack([has, page, slot]).astype(jnp.int32)


def lane_limits(contexts, lengths):
    lane = np.arange(DL, dtype=np.int32)
    row = np.arange(PPG, dtype=np.int32)[:, None] * HALF_GRP + lane % HALF_GRP
    spare = (lane % DH >= STEPS * HALF_GRP)[None, :]
    prompt = np.broadcast_to(np.arange(PPG, dtype=np.int32)[:, None], (PPG, DL))
    limits = jnp.minimum(lookup(contexts, row), lookup(lengths, prompt))
    return jnp.where(spare, 0, limits).reshape(PPG, 1, DL)


def absorb_queries(q_ref, dq_ref, u_ref, qt_ref, dqt_ref):
    for p in range(PPG):
        for a in range(2):
            rows = []
            for h in range(HEADS):
                cols = slice(h * HEAD, (h + 1) * HEAD)
                rows.append(
                    lax.dot_general(
                        q_ref[p, a * BLOCK : (a + 1) * BLOCK, cols],
                        u_ref[:, cols],
                        (((1,), (1,)), ((), ())),
                        preferred_element_type=jnp.float32,
                    )
                )
            qt_ref[p * 2 + a] = jnp.concatenate(rows, axis=0).T.astype(jnp.bfloat16)
        rows = []
        for h in range(HEADS):
            cols = slice(h * HEAD, (h + 1) * HEAD)
            q = jnp.concatenate(
                [dq_ref[t, p * HALF_GRP : (p + 1) * HALF_GRP, cols] for t in range(STEPS)]
                + [jnp.zeros((HALF_GRP, HEAD), jnp.bfloat16)],
                axis=0,
            )
            rows.append(
                lax.dot_general(
                    q, u_ref[:, cols], (((1,), (1,)), ((), ())), preferred_element_type=jnp.float32
                )
            )
        dqt_ref[p] = jnp.concatenate(rows, axis=0).T.astype(jnp.bfloat16)


def take_scores(k, q, keep_of, s_ref, peak_ref, p):
    s = jnp.dot(k, q, preferred_element_type=jnp.float32)
    peak = None
    for j in range(G):
        rows = slice(j * BLOCK, (j + 1) * BLOCK)
        part = jnp.where(keep_of(j), s[rows], NEG)
        s_ref[p, rows] = part
        top = jnp.max(part, axis=0, keepdims=True)
        peak = top if peak is None else jnp.maximum(peak, top)
    peak_ref[p] = peak


def weights_of(s_ref, peak_ref, p, m_ref, l_ref, at):
    old = m_ref[at]
    new = jnp.maximum(old, peak_ref[p] * SCALE2)
    factor = jnp.exp2(old - new)
    total = l_ref[at] * factor
    parts = []
    for j in range(G):
        w = jnp.exp2(s_ref[p, j * BLOCK : (j + 1) * BLOCK] * SCALE2 - new)
        total = total + jnp.sum(w, axis=0, keepdims=True)
        parts.append(w.astype(jnp.bfloat16))
    m_ref[at] = new
    l_ref[at] = total
    return jnp.concatenate(parts, axis=0), factor


def weigh(v, w, factor, acc_ref, at):
    part = lax.dot_general(v, w, (((0,), (0,)), ((), ())), preferred_element_type=jnp.float32)
    acc_ref[at] = acc_ref[at] * factor + part


def chunk_kernel(chunk, n_src, sizes, first, last, *refs):
    refs = list(refs)
    order, lengths, contexts = refs.pop(0), refs.pop(0), refs.pop(0)
    pages = refs.pop(0)
    mine = [refs.pop(0) for _ in range(n_src)]
    theirs = [refs.pop(0) for _ in range(n_src)]
    limit = refs.pop(0)
    if first:
        new_mine, new_theirs, q_in, dq_in, key_up = [refs.pop(0) for _ in range(5)]
    else:
        qt, dqt = refs.pop(0), refs.pop(0)
        state_in = [refs.pop(0) for _ in range(6)]
    if last:
        vup = refs.pop(0)
    if not first:
        refs.pop(0)
    if last:
        out_ref, dec_ref = refs.pop(0), refs.pop(0)
    else:
        state_out = [refs.pop(0) for _ in range(6)]
        if first:
            qt, dqt = refs.pop(0), refs.pop(0)
    cache_ref = refs.pop(0)
    kbuf, vbuf, sbuf, dsbuf, peak, dpeak, offset, place, sems = [refs.pop(0) for _ in range(9)]
    page_sems = refs.pop(0)
    if last:
        state = state_in
    else:
        state = state_out
    m, l, acc, dm, dl, dacc = state

    sec, ci = lax.axis_index("sec"), lax.axis_index("cp")
    z, y = ci // YN, lax.rem(ci, YN)
    spans, at = [], 0
    for n in sizes:
        spans.append((at, n))
        at += n

    def copies(k_src, v_src):
        made = []
        for i, (start, n) in enumerate(spans):
            made.append(pltpu.make_async_copy(k_src[i], kbuf.at[pl.ds(start, n)], sems.at[2 * i]))
            made.append(pltpu.make_async_copy(v_src[i], vbuf.at[pl.ds(start, n)], sems.at[2 * i + 1]))
        return made

    @pl.when(sec == 0)
    def _():
        for copy in copies(mine, theirs):
            copy.start()

    @pl.when(sec != 0)
    def _():
        for copy in copies(theirs, mine):
            copy.start()

    sources = []
    for i, dz in enumerate(CHUNK_Z[chunk]):
        sources += [(dz, dy, i, 4 * dy) for dy in range(YN)]
    if last:
        sources = [(4, 2 * i + e, i, 4 * e) for i in range(2) for e in range(2)]

    def page_copies(n, dz, dy, i, base):
        s = lax.rem(z + dz, ZN) * YN + lax.rem(y + dy, YN)
        page, slot = pages[PG_K, s], pages[PG_SLOT, s]
        block = base + page // 6
        row = pl.ds(pl.multiple_of(lax.rem(page, 6) * PAGE, PAGE), PAGE)
        rows = pl.ds(pl.multiple_of(jnp.minimum(slot, PAGES_DEV - 1) * PAGE, PAGE), PAGE)
        made = []
        for src, half, at in ((mine[i], sec, 2 * n), (theirs[i], 1 - sec, 2 * n + 1)):
            cols = pl.ds(pl.multiple_of(half * RANK, RANK), RANK)
            made.append(pltpu.make_async_copy(src.at[block, row, :], cache_ref.at[rows, cols], page_sems.at[at]))
        return pages[PG_HAS, s] > 0, made

    for n, entry in enumerate(sources):
        has, made = page_copies(n, *entry)

        @pl.when(has)
        def _(made=made):
            for copy in made:
                copy.start()

    slots = [j for j in range(16) if SLOT_OK[chunk, j]]
    orders = []
    for j in slots:
        source = lax.rem(z + int(SLOT_Z[chunk, j]), ZN) * YN + lax.rem(y + int(SLOT_Y[chunk, j]), YN)
        orders.append(order[2 * source + int(SLOT_A[chunk, j])])
    ranks = [jnp.int32(0)] * len(slots)
    for i in range(len(slots)):
        for j in range(i):
            ahead = jnp.where(orders[j] < orders[i], 1, 0)
            ranks[i], ranks[j] = ranks[i] + ahead, ranks[j] + 1 - ahead
    for i, j in enumerate(slots):
        place[ranks[i]] = jnp.int32(int(SLOT_ROW[chunk, j]))
        place[16 + ranks[i]] = orders[i]
    owns = [order[2 * ci + a] for a in range(2)]
    longest = jnp.maximum(lengths[0], lengths[1])
    reach = jnp.int32(0)
    for n in range(ROW_GRP):
        reach = jnp.maximum(reach, jnp.minimum(contexts[n], lengths[n // HALF_GRP]))
    every = []
    for a in range(2):
        count = jnp.int32(0)
        for one in orders:
            count = count + jnp.where(one <= owns[a], 1, 0)
        every.append(jnp.where(owns[a] * BLOCK < longest, count, 0))
    dec_count = jnp.int32(0)
    for one in orders:
        dec_count = dec_count + jnp.where(one * BLOCK < reach, 1, 0)

    if first:
        absorb_queries(q_in, dq_in, key_up, qt, dqt)
        m[...] = jnp.full(m.shape, NEG, jnp.float32)
        l[...] = jnp.zeros(l.shape, jnp.float32)
        acc[...] = jnp.zeros(acc.shape, jnp.float32)
        is_key = sec == 0
        lane = lax.broadcasted_iota(jnp.int32, (1, DL), 1)
        step_of = lax.rem(lane, DH) // HALF_GRP
        for p in range(PPG):
            scores, values = [], []
            for t in range(STEPS):
                rows = slice(t * ROW_GRP + p * HALF_GRP, t * ROW_GRP + (p + 1) * HALF_GRP)
                a, b = new_mine[rows, :].astype(jnp.float32), new_theirs[rows, :].astype(jnp.float32)
                k, v = jnp.where(is_key, a, b), jnp.where(is_key, b, a)
                k = jnp.concatenate([k] * (DL // HALF_GRP), axis=0).T
                values.append(jnp.concatenate([v] * (DL // HALF_GRP), axis=0).T)
                s = jnp.sum(dqt[p].astype(jnp.float32) * k, axis=0, keepdims=True) * SCALE2
                scores.append(jnp.where(t <= step_of, s, NEG))
            top = jnp.maximum(jnp.maximum(scores[0], scores[1]), scores[2])
            weights = [jnp.exp2(s - top) for s in scores]
            dm[p] = top
            dl[p] = weights[0] + weights[1] + weights[2]
            total = jnp.zeros((RANK, DL), jnp.float32)
            for w, v in zip(weights, values):
                total = total + w.astype(jnp.bfloat16).astype(jnp.float32) * v
            dacc[p] = total
    elif not last:
        for src, dst in zip(state_in, state_out):
            dst[...] = src[...]

    for copy in copies(mine, theirs):
        copy.wait()

    def rows_of(buf, g, p):
        return jnp.concatenate([buf[place[g * G + j] + 2 * p] for j in range(G)], axis=0)

    key_row = lax.broadcasted_iota(jnp.int32, (BLOCK, QL), 0)
    query_row = lax.rem(lax.broadcasted_iota(jnp.int32, (BLOCK, QL), 1), BLOCK)
    offset[...] = key_row - query_row
    groups = [(every[a] + G - 1) // G for a in range(2)]
    work = groups[0] + groups[1]

    def part_of(w):
        a = jnp.where(w >= groups[0], 1, 0)
        return a, w - a * groups[0]

    def scores(w, p):
        a, g = part_of(w)
        own = jnp.where(a == 0, owns[0], owns[1])

        def keep_of(j):
            return offset[...] <= (own - place[16 + g * G + j]) * BLOCK

        take_scores(rows_of(kbuf, g, p), qt[2 * p + a], keep_of, sbuf, peak, p)

    @pl.when(work > 0)
    def _():
        for p in range(PPG):
            scores(0, p)

    def step(w, carry):
        a, g = part_of(w)
        after = jnp.minimum(w + 1, work - 1)
        for p in range(PPG):
            weights, factor = weights_of(sbuf, peak, p, m, l, 2 * p + a)
            scores(after, p)
            weigh(rows_of(vbuf, g, p), weights, factor, acc, 2 * p + a)
        return carry

    lax.fori_loop(0, work, step, 0)

    dec_row = lax.broadcasted_iota(jnp.int32, (BLOCK, DL), 0)
    dec_work = (dec_count + G - 1) // G

    def dec_scores(g, p):
        def keep_of(j):
            return dec_row < limit[p] - place[16 + g * G + j] * BLOCK

        take_scores(rows_of(kbuf, g, p), dqt[p], keep_of, dsbuf, dpeak, p)

    @pl.when(dec_work > 0)
    def _():
        for p in range(PPG):
            dec_scores(0, p)

    def dec_step(g, carry):
        after = jnp.minimum(g + 1, dec_work - 1)
        for p in range(PPG):
            weights, factor = weights_of(dsbuf, dpeak, p, dm, dl, p)
            dec_scores(after, p)
            weigh(rows_of(vbuf, g, p), weights, factor, dacc, p)
        return carry

    lax.fori_loop(0, dec_work, dec_step, 0)

    if last:
        row = lax.broadcasted_iota(jnp.int32, (BLOCK, HEAD), 0)
        for p in range(PPG):
            for a in range(2):
                at = p * 2 + a
                o = (acc[at] * (1.0 / l[at])).T.astype(jnp.bfloat16)
                live = row + owns[a] * BLOCK < lengths[p]
                for h in range(HEADS):
                    cols = slice(h * HEAD, (h + 1) * HEAD)
                    r = jnp.dot(
                        o[h * BLOCK : (h + 1) * BLOCK], vup[:, cols], preferred_element_type=jnp.float32
                    )
                    out_ref[p, a * BLOCK : (a + 1) * BLOCK, cols] = jnp.where(live, r, 0.0).astype(
                        jnp.bfloat16
                    )
            o = (dacc[p] * (1.0 / dl[p])).T.astype(jnp.bfloat16)
            for h in range(HEADS):
                cols = slice(h * HEAD, (h + 1) * HEAD)
                r = jnp.dot(
                    o[h * DH : (h + 1) * DH], vup[:, cols], preferred_element_type=jnp.float32
                ).astype(jnp.bfloat16)
                for t in range(STEPS):
                    dec_ref[t, p * HALF_GRP : (p + 1) * HALF_GRP, cols] = r[t * HALF_GRP : (t + 1) * HALF_GRP]

    for n, entry in enumerate(sources):
        has, made = page_copies(n, *entry)

        @pl.when(has)
        def _(made=made):
            for copy in made:
                copy.wait()


STATE = (
    jax.ShapeDtypeStruct((UNITS, 1, QL), jnp.float32),
    jax.ShapeDtypeStruct((UNITS, 1, QL), jnp.float32),
    jax.ShapeDtypeStruct((UNITS, RANK, QL), jnp.float32),
    jax.ShapeDtypeStruct((PPG, 1, DL), jnp.float32),
    jax.ShapeDtypeStruct((PPG, 1, DL), jnp.float32),
    jax.ShapeDtypeStruct((PPG, RANK, DL), jnp.float32),
)


QUERIES = (
    jax.ShapeDtypeStruct((UNITS, RANK, QL), jnp.bfloat16),
    jax.ShapeDtypeStruct((PPG, RANK, DL), jnp.bfloat16),
)


def attend_chunk(chunk, control, mine, theirs, limit, queries=None, state=None, start=None, value_up=None):
    first, last = state is None, value_up is not None
    smem, vmem = pl.BlockSpec(memory_space=pltpu.SMEM), pl.BlockSpec(memory_space=pltpu.VMEM)
    anywhere = pl.BlockSpec(memory_space=pl.ANY)
    sizes = [a.size // (BLOCK * RANK) for a in mine]
    flat = [a.reshape(-1, BLOCK, RANK) for a in [*mine, *theirs]]
    args, specs = list(control), [smem] * 4
    args, specs = args + flat, specs + [anywhere] * len(flat)
    args, specs = args + [limit], specs + [vmem]
    if first:
        args, specs = args + list(start), specs + [vmem] * 5
    else:
        *state, cache = state
        args, specs = args + list(queries) + list(state), specs + [vmem] * 8
    if last:
        args, specs = args + [value_up], specs + [vmem]
    if not first:
        args, specs = args + [cache], specs + [anywhere]
    rows = sum(sizes)
    scratch = [
        pltpu.VMEM((rows, BLOCK, RANK), jnp.bfloat16),
        pltpu.VMEM((rows, BLOCK, RANK), jnp.bfloat16),
        pltpu.VMEM((PPG, GK, QL), jnp.float32),
        pltpu.VMEM((PPG, GK, DL), jnp.float32),
        pltpu.VMEM((PPG, 1, QL), jnp.float32),
        pltpu.VMEM((PPG, 1, DL), jnp.float32),
        pltpu.VMEM((BLOCK, QL), jnp.int32),
        pltpu.SMEM((32,), jnp.int32),
        pltpu.SemaphoreType.DMA((2 * len(mine),)),
    ]
    scratch.append(pltpu.SemaphoreType.DMA((2 * (2 * rows // 8),)))
    if last:
        shapes = (
            jax.ShapeDtypeStruct((PPG, 2 * BLOCK, HEADS * HEAD), jnp.bfloat16),
            jax.ShapeDtypeStruct((STEPS, ROW_GRP, HEADS * HEAD), jnp.bfloat16),
        )
    else:
        shapes = STATE + QUERIES if first else STATE
    out_specs = [vmem] * len(shapes) + [anywhere]
    shapes += (jax.ShapeDtypeStruct((PAGES_DEV * PAGE, 2 * RANK), jnp.bfloat16),)
    work = rows * BLOCK * (2 * QL + DL) * RANK * 4
    return pl.pallas_call(
        functools.partial(chunk_kernel, chunk, len(mine), sizes, first, last),
        out_shape=shapes,
        in_specs=specs,
        out_specs=out_specs,
        scratch_shapes=scratch,
        input_output_aliases={} if first else {len(args) - 1: len(shapes) - 1},
        cost_estimate=pl.CostEstimate(flops=2 * work, bytes_accessed=4 * 10**6, transcendentals=work // 512),
        compiler_params=pltpu.CompilerParams(vmem_limit_bytes=20 * 2**20),
    )(*args)


def project_kernel(x_ref, w_ref, out_ref, total):
    k = pl.program_id(0)
    part = jnp.dot(x_ref[...], w_ref[...], preferred_element_type=jnp.float32)

    @pl.when(k == 0)
    def _():
        total[...] = part

    @pl.when(k > 0)
    def _():
        total[...] += part

    @pl.when(k == pl.num_programs(0) - 1)
    def _():
        out_ref[...] = total[...].astype(jnp.bfloat16)


def project(x, w, parts=8):
    rows, width = x.shape
    depth = width // parts
    return pl.pallas_call(
        project_kernel,
        grid=(parts,),
        out_shape=jax.ShapeDtypeStruct((rows, RANK), jnp.bfloat16),
        in_specs=[
            pl.BlockSpec((rows, depth), lambda k: (0, k)),
            pl.BlockSpec((depth, RANK), lambda k: (k, 0)),
        ],
        out_specs=pl.BlockSpec((rows, RANK), lambda k: (0, 0)),
        scratch_shapes=[pltpu.VMEM((rows, RANK), jnp.float32)],
        cost_estimate=pl.CostEstimate(
            flops=2 * rows * width * RANK, bytes_accessed=2 * width * (rows + RANK), transcendentals=0
        ),
        compiler_params=pltpu.CompilerParams(vmem_limit_bytes=8 * 2**20),
        name="project",
    )(x, w)


def shifted(x, dz, dy):
    pairs = [
        (z * YN + y, ((z + dz) % ZN) * YN + (y + dy) % YN) for z in range(ZN) for y in range(YN)
    ]
    return lax.ppermute(x, "cp", pairs)


def swapped(x):
    return lax.ppermute(x, "sec", [(0, 1), (1, 0)])


def body(
    prompt_states,
    prompt_queries,
    decode_states,
    decode_queries,
    latent_down,
    key_up,
    value_up,
    prompt_lengths,
    block_order,
    page_owner,
    decode_context,
):
    width = prompt_states.shape[-1]
    ci = lax.axis_index("cp")
    own = project(prompt_states.reshape(PPG * 2 * BLOCK, width), latent_down)
    own = own.reshape(UNITS, BLOCK, RANK)
    new = jnp.dot(
        decode_states.reshape(STEPS * ROW_GRP, width), latent_down, preferred_element_type=jnp.float32
    ).astype(jnp.bfloat16)
    control = (block_order, prompt_lengths, decode_context, page_table(page_owner[0], ci))
    limit = lane_limits(decode_context, prompt_lengths)

    plane = jnp.stack([own, shifted(own, 0, -1), shifted(own, 0, 2), shifted(own, 0, 1)])
    new_far = swapped(new)
    up, down = shifted(plane, 1, 0), shifted(plane, -1, 0)
    plane_far = swapped(plane)
    start = (new, new_far, prompt_queries, decode_queries, key_up)
    *state, qt, dqt, cache = attend_chunk(0, control, [plane], [plane_far], limit, start=start)
    state = [*state, cache]
    for c in range(1, 4):
        if c < 3:
            up_next = shifted(up, 1, 0)
            down_next = shifted(down, -1, 0)
        else:
            up_next = shifted(up[:2], 1, 0)
            down_next = shifted(down[2:], -1, 0)
        up_far, down_far = swapped(up), swapped(down)
        state = attend_chunk(
            c, control, [up, down], [up_far, down_far], limit, queries=(qt, dqt), state=state
        )
        up, down = up_next, down_next
    far = [swapped(up), swapped(down)]
    prefill_out, decode_out, cache = attend_chunk(
        4, control, [up, down], far, limit, queries=(qt, dqt), state=state, value_up=value_up
    )
    return prefill_out, decode_out, cache.reshape(1, 1, PAGES_DEV * PAGE, 2 * RANK)


def solution(mesh):
    placed = (
        P("grp", "cp", None),
        P("grp", "cp", "sec"),
        P(None, "grp", None),
        P(None, "grp", "sec"),
        P(None, "sec"),
        P(None, "sec"),
        P(None, "sec"),
        P("grp"),
        P(),
        P("grp", None, None),
        P("grp"),
    )
    return jax.shard_map(
        body,
        mesh=mesh,
        in_specs=placed,
        out_specs=(P("grp", "cp", "sec"), P(None, "grp", "sec"), P("grp", "cp", None, None)),
        check_vma=False,
    )
```

```python
import functools
import math

import jax
import jax.numpy as jnp
import numpy as np
from jax import lax
from jax.experimental import pallas as pl
from jax.experimental.pallas import tpu as pltpu
from jax.sharding import PartitionSpec as P


HEAD = 128
RANK = 128
HEADS = 4
BLOCK = 96
PAGE = 16
PPG = 2
ROW_GRP = 32
HALF_GRP = ROW_GRP // PPG
STEPS = 3
PAGES_DEV = 24
ZN, YN = 8, 4
CP = ZN * YN
UNITS = 4
QL = HEADS * BLOCK
DH = 64
DL = HEADS * DH
G = 4
GK = G * BLOCK
NEG = -1e30
SCALE2 = math.log2(math.e) / math.sqrt(HEAD)

CHUNK_Z = [[0], [7, 1], [6, 2], [5, 3], [4]]
SLOT_Z = np.zeros((5, 16), np.int32)
SLOT_Y = np.zeros((5, 16), np.int32)
SLOT_A = np.zeros((5, 16), np.int32)
SLOT_ROW = np.zeros((5, 16), np.int32)
SLOT_OK = np.zeros((5, 16), bool)
for _c, _zs in enumerate(CHUNK_Z):
    for _i, _dz in enumerate(_zs):
        for _dy in range(YN):
            for _a in range(2):
                _j = _i * 8 + _dy * 2 + _a
                SLOT_Z[_c, _j], SLOT_Y[_c, _j], SLOT_A[_c, _j] = _dz, _dy, _a
                SLOT_ROW[_c, _j] = _i * 16 + _dy * 4 + _a
                SLOT_OK[_c, _j] = True

PG_HAS, PG_K, PG_SLOT = 0, 1, 2


def lookup(table, indices):
    matches = indices[..., None] == jnp.arange(table.shape[0], dtype=jnp.int32)
    return jnp.sum(jnp.where(matches, table, 0), axis=-1)


def page_table(owners, ci):
    mine = owners == ci
    has = jnp.sum(mine.astype(jnp.int32), axis=1)
    page = jnp.sum(jnp.where(mine, np.arange(PAGES_DEV, dtype=np.int32), 0), axis=1)
    before = np.arange(CP)[None, :] < np.arange(CP)[:, None]
    slot = jnp.sum(jnp.where(before, has[None, :], 0), axis=1)
    return jnp.stack([has, page, slot]).astype(jnp.int32)


def lane_limits(contexts, lengths):
    lane = np.arange(DL, dtype=np.int32)
    row = np.arange(PPG, dtype=np.int32)[:, None] * HALF_GRP + lane % HALF_GRP
    spare = (lane % DH >= STEPS * HALF_GRP)[None, :]
    prompt = np.broadcast_to(np.arange(PPG, dtype=np.int32)[:, None], (PPG, DL))
    limits = jnp.minimum(lookup(contexts, row), lookup(lengths, prompt))
    return jnp.where(spare, 0, limits).reshape(PPG, 1, DL)


def absorb_queries(q_ref, dq_ref, u_ref, qt_ref, dqt_ref):
    for p in range(PPG):
        for a in range(2):
            rows = []
            for h in range(HEADS):
                cols = slice(h * HEAD, (h + 1) * HEAD)
                rows.append(
                    lax.dot_general(
                        q_ref[p, a * BLOCK : (a + 1) * BLOCK, cols],
                        u_ref[:, cols],
                        (((1,), (1,)), ((), ())),
                        preferred_element_type=jnp.float32,
                    )
                )
            qt_ref[p * 2 + a] = jnp.concatenate(rows, axis=0).T.astype(jnp.bfloat16)
        rows = []
        for h in range(HEADS):
            cols = slice(h * HEAD, (h + 1) * HEAD)
            q = jnp.concatenate(
                [dq_ref[t, p * HALF_GRP : (p + 1) * HALF_GRP, cols] for t in range(STEPS)]
                + [jnp.zeros((HALF_GRP, HEAD), jnp.bfloat16)],
                axis=0,
            )
            rows.append(
                lax.dot_general(
                    q, u_ref[:, cols], (((1,), (1,)), ((), ())), preferred_element_type=jnp.float32
                )
            )
        dqt_ref[p] = jnp.concatenate(rows, axis=0).T.astype(jnp.bfloat16)


def take_scores(k, q, keep_of, s_ref, peak_ref, p):
    s = jnp.dot(k, q, preferred_element_type=jnp.float32)
    peak = None
    for j in range(G):
        rows = slice(j * BLOCK, (j + 1) * BLOCK)
        part = jnp.where(keep_of(j), s[rows], NEG)
        s_ref[p, rows] = part
        top = jnp.max(part, axis=0, keepdims=True)
        peak = top if peak is None else jnp.maximum(peak, top)
    peak_ref[p] = peak


def weights_of(s_ref, peak_ref, p, m_ref, l_ref, at):
    old = m_ref[at]
    new = jnp.maximum(old, peak_ref[p] * SCALE2)
    factor = jnp.exp2(old - new)
    total = l_ref[at] * factor
    parts = []
    for j in range(G):
        w = jnp.exp2(s_ref[p, j * BLOCK : (j + 1) * BLOCK] * SCALE2 - new)
        total = total + jnp.sum(w, axis=0, keepdims=True)
        parts.append(w.astype(jnp.bfloat16))
    m_ref[at] = new
    l_ref[at] = total
    return jnp.concatenate(parts, axis=0), factor


def weigh(v, w, factor, acc_ref, at):
    part = lax.dot_general(v, w, (((0,), (0,)), ((), ())), preferred_element_type=jnp.float32)
    acc_ref[at] = acc_ref[at] * factor + part


def chunk_kernel(chunk, n_src, sizes, first, last, *refs):
    refs = list(refs)
    order, lengths, contexts = refs.pop(0), refs.pop(0), refs.pop(0)
    pages = refs.pop(0)
    mine = [refs.pop(0) for _ in range(n_src)]
    theirs = [refs.pop(0) for _ in range(n_src)]
    limit = refs.pop(0)
    if first:
        new_mine, new_theirs, q_in, dq_in, key_up = [refs.pop(0) for _ in range(5)]
    else:
        qt, dqt = refs.pop(0), refs.pop(0)
        state_in = [refs.pop(0) for _ in range(6)]
    if last:
        vup = refs.pop(0)
    if not first:
        refs.pop(0)
    if last:
        out_ref, dec_ref = refs.pop(0), refs.pop(0)
    else:
        state_out = [refs.pop(0) for _ in range(6)]
        if first:
            qt, dqt = refs.pop(0), refs.pop(0)
    cache_ref = refs.pop(0)
    kbuf, vbuf, sbuf, dsbuf, peak, dpeak, offset, place, sems = [refs.pop(0) for _ in range(9)]
    page_sems = refs.pop(0)
    if last:
        state = state_in
    else:
        state = state_out
    m, l, acc, dm, dl, dacc = state

    sec, ci = lax.axis_index("sec"), lax.axis_index("cp")
    z, y = ci // YN, lax.rem(ci, YN)
    spans, at = [], 0
    for n in sizes:
        spans.append((at, n))
        at += n

    def copies(k_src, v_src):
        made = []
        for i, (start, n) in enumerate(spans):
            made.append(pltpu.make_async_copy(k_src[i], kbuf.at[pl.ds(start, n)], sems.at[2 * i]))
            made.append(pltpu.make_async_copy(v_src[i], vbuf.at[pl.ds(start, n)], sems.at[2 * i + 1]))
        return made

    @pl.when(sec == 0)
    def _():
        for copy in copies(mine, theirs):
            copy.start()

    @pl.when(sec != 0)
    def _():
        for copy in copies(theirs, mine):
            copy.start()

    sources = []
    for i, dz in enumerate(CHUNK_Z[chunk]):
        sources += [(dz, dy, i, 4 * dy) for dy in range(YN)]
    if last:
        sources = [(4, 2 * i + e, i, 4 * e) for i in range(2) for e in range(2)]

    def page_copies(n, dz, dy, i, base):
        s = lax.rem(z + dz, ZN) * YN + lax.rem(y + dy, YN)
        page, slot = pages[PG_K, s], pages[PG_SLOT, s]
        block = base + page // 6
        row = pl.ds(pl.multiple_of(lax.rem(page, 6) * PAGE, PAGE), PAGE)
        rows = pl.ds(pl.multiple_of(jnp.minimum(slot, PAGES_DEV - 1) * PAGE, PAGE), PAGE)
        made = []
        for src, half, at in ((mine[i], sec, 2 * n), (theirs[i], 1 - sec, 2 * n + 1)):
            cols = pl.ds(pl.multiple_of(half * RANK, RANK), RANK)
            made.append(pltpu.make_async_copy(src.at[block, row, :], cache_ref.at[rows, cols], page_sems.at[at]))
        return pages[PG_HAS, s] > 0, made

    for n, entry in enumerate(sources):
        has, made = page_copies(n, *entry)

        @pl.when(has)
        def _(made=made):
            for copy in made:
                copy.start()

    slots = [j for j in range(16) if SLOT_OK[chunk, j]]
    orders = []
    for j in slots:
        source = lax.rem(z + int(SLOT_Z[chunk, j]), ZN) * YN + lax.rem(y + int(SLOT_Y[chunk, j]), YN)
        orders.append(order[2 * source + int(SLOT_A[chunk, j])])
    ranks = [jnp.int32(0)] * len(slots)
    for i in range(len(slots)):
        for j in range(i):
            ahead = jnp.where(orders[j] < orders[i], 1, 0)
            ranks[i], ranks[j] = ranks[i] + ahead, ranks[j] + 1 - ahead
    for i, j in enumerate(slots):
        place[ranks[i]] = jnp.int32(int(SLOT_ROW[chunk, j]))
        place[16 + ranks[i]] = orders[i]
    owns = [order[2 * ci + a] for a in range(2)]
    longest = jnp.maximum(lengths[0], lengths[1])
    reach = jnp.int32(0)
    for n in range(ROW_GRP):
        reach = jnp.maximum(reach, jnp.minimum(contexts[n], lengths[n // HALF_GRP]))
    every = []
    for a in range(2):
        count = jnp.int32(0)
        for one in orders:
            count = count + jnp.where(one <= owns[a], 1, 0)
        every.append(jnp.where(owns[a] * BLOCK < longest, count, 0))
    dec_count = jnp.int32(0)
    for one in orders:
        dec_count = dec_count + jnp.where(one * BLOCK < reach, 1, 0)

    if first:
        absorb_queries(q_in, dq_in, key_up, qt, dqt)
        m[...] = jnp.full(m.shape, NEG, jnp.float32)
        l[...] = jnp.zeros(l.shape, jnp.float32)
        acc[...] = jnp.zeros(acc.shape, jnp.float32)
        is_key = sec == 0
        lane = lax.broadcasted_iota(jnp.int32, (1, DL), 1)
        step_of = lax.rem(lane, DH) // HALF_GRP
        for p in range(PPG):
            scores, values = [], []
            for t in range(STEPS):
                rows = slice(t * ROW_GRP + p * HALF_GRP, t * ROW_GRP + (p + 1) * HALF_GRP)
                a, b = new_mine[rows, :].astype(jnp.float32), new_theirs[rows, :].astype(jnp.float32)
                k, v = jnp.where(is_key, a, b), jnp.where(is_key, b, a)
                k = jnp.concatenate([k] * (DL // HALF_GRP), axis=0).T
                values.append(jnp.concatenate([v] * (DL // HALF_GRP), axis=0).T)
                s = jnp.sum(dqt[p].astype(jnp.float32) * k, axis=0, keepdims=True) * SCALE2
                scores.append(jnp.where(t <= step_of, s, NEG))
            top = jnp.maximum(jnp.maximum(scores[0], scores[1]), scores[2])
            weights = [jnp.exp2(s - top) for s in scores]
            dm[p] = top
            dl[p] = weights[0] + weights[1] + weights[2]
            total = jnp.zeros((RANK, DL), jnp.float32)
            for w, v in zip(weights, values):
                total = total + w.astype(jnp.bfloat16).astype(jnp.float32) * v
            dacc[p] = total
    elif not last:
        for src, dst in zip(state_in, state_out):
            dst[...] = src[...]

    for copy in copies(mine, theirs):
        copy.wait()

    def rows_of(buf, g, p):
        return jnp.concatenate([buf[place[g * G + j] + 2 * p] for j in range(G)], axis=0)

    key_row = lax.broadcasted_iota(jnp.int32, (BLOCK, QL), 0)
    query_row = lax.rem(lax.broadcasted_iota(jnp.int32, (BLOCK, QL), 1), BLOCK)
    offset[...] = key_row - query_row
    groups = [(every[a] + G - 1) // G for a in range(2)]
    work = groups[0] + groups[1]

    def part_of(w):
        a = jnp.where(w >= groups[0], 1, 0)
        return a, w - a * groups[0]

    def scores(w, p):
        a, g = part_of(w)
        own = jnp.where(a == 0, owns[0], owns[1])

        def keep_of(j):
            return offset[...] <= (own - place[16 + g * G + j]) * BLOCK

        take_scores(rows_of(kbuf, g, p), qt[2 * p + a], keep_of, sbuf, peak, p)

    @pl.when(work > 0)
    def _():
        for p in range(PPG):
            scores(0, p)

    def step(w, carry):
        a, g = part_of(w)
        after = jnp.minimum(w + 1, work - 1)
        for p in range(PPG):
            weights, factor = weights_of(sbuf, peak, p, m, l, 2 * p + a)
            scores(after, p)
            weigh(rows_of(vbuf, g, p), weights, factor, acc, 2 * p + a)
        return carry

    lax.fori_loop(0, work, step, 0)

    dec_row = lax.broadcasted_iota(jnp.int32, (BLOCK, DL), 0)
    dec_work = (dec_count + G - 1) // G

    def dec_scores(g, p):
        def keep_of(j):
            return dec_row < limit[p] - place[16 + g * G + j] * BLOCK

        take_scores(rows_of(kbuf, g, p), dqt[p], keep_of, dsbuf, dpeak, p)

    @pl.when(dec_work > 0)
    def _():
        for p in range(PPG):
            dec_scores(0, p)

    def dec_step(g, carry):
        after = jnp.minimum(g + 1, dec_work - 1)
        for p in range(PPG):
            weights, factor = weights_of(dsbuf, dpeak, p, dm, dl, p)
            dec_scores(after, p)
            weigh(rows_of(vbuf, g, p), weights, factor, dacc, p)
        return carry

    lax.fori_loop(0, dec_work, dec_step, 0)

    if last:
        row = lax.broadcasted_iota(jnp.int32, (BLOCK, HEAD), 0)
        for p in range(PPG):
            for a in range(2):
                at = p * 2 + a
                o = (acc[at] * (1.0 / l[at])).T.astype(jnp.bfloat16)
                live = row + owns[a] * BLOCK < lengths[p]
                for h in range(HEADS):
                    cols = slice(h * HEAD, (h + 1) * HEAD)
                    r = jnp.dot(
                        o[h * BLOCK : (h + 1) * BLOCK], vup[:, cols], preferred_element_type=jnp.float32
                    )
                    out_ref[p, a * BLOCK : (a + 1) * BLOCK, cols] = jnp.where(live, r, 0.0).astype(
                        jnp.bfloat16
                    )
            o = (dacc[p] * (1.0 / dl[p])).T.astype(jnp.bfloat16)
            for h in range(HEADS):
                cols = slice(h * HEAD, (h + 1) * HEAD)
                r = jnp.dot(
                    o[h * DH : (h + 1) * DH], vup[:, cols], preferred_element_type=jnp.float32
                ).astype(jnp.bfloat16)
                for t in range(STEPS):
                    dec_ref[t, p * HALF_GRP : (p + 1) * HALF_GRP, cols] = r[t * HALF_GRP : (t + 1) * HALF_GRP]

    for n, entry in enumerate(sources):
        has, made = page_copies(n, *entry)

        @pl.when(has)
        def _(made=made):
            for copy in made:
                copy.wait()


STATE = (
    jax.ShapeDtypeStruct((UNITS, 1, QL), jnp.float32),
    jax.ShapeDtypeStruct((UNITS, 1, QL), jnp.float32),
    jax.ShapeDtypeStruct((UNITS, RANK, QL), jnp.float32),
    jax.ShapeDtypeStruct((PPG, 1, DL), jnp.float32),
    jax.ShapeDtypeStruct((PPG, 1, DL), jnp.float32),
    jax.ShapeDtypeStruct((PPG, RANK, DL), jnp.float32),
)


QUERIES = (
    jax.ShapeDtypeStruct((UNITS, RANK, QL), jnp.bfloat16),
    jax.ShapeDtypeStruct((PPG, RANK, DL), jnp.bfloat16),
)


def attend_chunk(chunk, control, mine, theirs, limit, queries=None, state=None, start=None, value_up=None):
    first, last = state is None, value_up is not None
    smem, vmem = pl.BlockSpec(memory_space=pltpu.SMEM), pl.BlockSpec(memory_space=pltpu.VMEM)
    anywhere = pl.BlockSpec(memory_space=pl.ANY)
    sizes = [a.size // (BLOCK * RANK) for a in mine]
    flat = [a.reshape(-1, BLOCK, RANK) for a in [*mine, *theirs]]
    args, specs = list(control), [smem] * 4
    args, specs = args + flat, specs + [anywhere] * len(flat)
    args, specs = args + [limit], specs + [vmem]
    if first:
        args, specs = args + list(start), specs + [vmem] * 5
    else:
        *state, cache = state
        args, specs = args + list(queries) + list(state), specs + [vmem] * 8
    if last:
        args, specs = args + [value_up], specs + [vmem]
    if not first:
        args, specs = args + [cache], specs + [anywhere]
    rows = sum(sizes)
    scratch = [
        pltpu.VMEM((rows, BLOCK, RANK), jnp.bfloat16),
        pltpu.VMEM((rows, BLOCK, RANK), jnp.bfloat16),
        pltpu.VMEM((PPG, GK, QL), jnp.float32),
        pltpu.VMEM((PPG, GK, DL), jnp.float32),
        pltpu.VMEM((PPG, 1, QL), jnp.float32),
        pltpu.VMEM((PPG, 1, DL), jnp.float32),
        pltpu.VMEM((BLOCK, QL), jnp.int32),
        pltpu.SMEM((32,), jnp.int32),
        pltpu.SemaphoreType.DMA((2 * len(mine),)),
    ]
    scratch.append(pltpu.SemaphoreType.DMA((2 * (2 * rows // 8),)))
    if last:
        shapes = (
            jax.ShapeDtypeStruct((PPG, 2 * BLOCK, HEADS * HEAD), jnp.bfloat16),
            jax.ShapeDtypeStruct((STEPS, ROW_GRP, HEADS * HEAD), jnp.bfloat16),
        )
    else:
        shapes = STATE + QUERIES if first else STATE
    out_specs = [vmem] * len(shapes) + [anywhere]
    shapes += (jax.ShapeDtypeStruct((PAGES_DEV * PAGE, 2 * RANK), jnp.bfloat16),)
    work = rows * BLOCK * (2 * QL + DL) * RANK * 4
    return pl.pallas_call(
        functools.partial(chunk_kernel, chunk, len(mine), sizes, first, last),
        out_shape=shapes,
        in_specs=specs,
        out_specs=out_specs,
        scratch_shapes=scratch,
        input_output_aliases={} if first else {len(args) - 1: len(shapes) - 1},
        cost_estimate=pl.CostEstimate(flops=2 * work, bytes_accessed=4 * 10**6, transcendentals=work // 512),
        compiler_params=pltpu.CompilerParams(vmem_limit_bytes=20 * 2**20),
    )(*args)


def shifted(x, dz, dy):
    pairs = [
        (z * YN + y, ((z + dz) % ZN) * YN + (y + dy) % YN) for z in range(ZN) for y in range(YN)
    ]
    return lax.ppermute(x, "cp", pairs)


def swapped(x):
    return lax.ppermute(x, "sec", [(0, 1), (1, 0)])


def body(
    prompt_states,
    prompt_queries,
    decode_states,
    decode_queries,
    latent_down,
    key_up,
    value_up,
    prompt_lengths,
    block_order,
    page_owner,
    decode_context,
):
    width = prompt_states.shape[-1]
    ci = lax.axis_index("cp")
    own = jnp.dot(
        prompt_states.reshape(PPG * 2 * BLOCK, width), latent_down, preferred_element_type=jnp.float32
    )
    own = own.astype(jnp.bfloat16).reshape(UNITS, BLOCK, RANK)
    new = jnp.dot(
        decode_states.reshape(STEPS * ROW_GRP, width), latent_down, preferred_element_type=jnp.float32
    ).astype(jnp.bfloat16)
    control = (block_order, prompt_lengths, decode_context, page_table(page_owner[0], ci))
    limit = lane_limits(decode_context, prompt_lengths)

    plane = jnp.stack([own, shifted(own, 0, -1), shifted(own, 0, 2), shifted(own, 0, 1)])
    new_far = swapped(new)
    up, down = shifted(plane, 1, 0), shifted(plane, -1, 0)
    plane_far = swapped(plane)
    start = (new, new_far, prompt_queries, decode_queries, key_up)
    *state, qt, dqt, cache = attend_chunk(0, control, [plane], [plane_far], limit, start=start)
    state = [*state, cache]
    for c in range(1, 4):
        if c < 3:
            up_next = shifted(up, 1, 0)
            down_next = shifted(down, -1, 0)
        else:
            up_next = shifted(up[:2], 1, 0)
            down_next = shifted(down[2:], -1, 0)
        up_far, down_far = swapped(up), swapped(down)
        state = attend_chunk(
            c, control, [up, down], [up_far, down_far], limit, queries=(qt, dqt), state=state
        )
        up, down = up_next, down_next
    far = [swapped(up), swapped(down)]
    prefill_out, decode_out, cache = attend_chunk(
        4, control, [up, down], far, limit, queries=(qt, dqt), state=state, value_up=value_up
    )
    return prefill_out, decode_out, cache.reshape(1, 1, PAGES_DEV * PAGE, 2 * RANK)


def solution(mesh):
    placed = (
        P("grp", "cp", None),
        P("grp", "cp", "sec"),
        P(None, "grp", None),
        P(None, "grp", "sec"),
        P(None, "sec"),
        P(None, "sec"),
        P(None, "sec"),
        P("grp"),
        P(),
        P("grp", None, None),
        P("grp"),
    )
    return jax.shard_map(
        body,
        mesh=mesh,
        in_specs=placed,
        out_specs=(P("grp", "cp", "sec"), P(None, "grp", "sec"), P("grp", "cp", None, None)),
        check_vma=False,
    )
```
